32 devices in a mesh: row: 4 (over x, core), col: 8 (over z, y).
Axes of the slice: x: 2, y: 2, z: 4, core: 2. Of those that a mesh axis runs over, the one named last changes fastest.
Arguments:
- rows: bfloat16 [1024, 4096], P(('row', 'col')), may hold values from -6 to 6
- task_ids: int32 [1024], P(('row', 'col')), may hold values from 0 to 8, as said below
- task_embed: bfloat16 [8, 4096], replicated, may hold values from -6 to 6
- norm_gain: float32 [4, 4096], replicated, may hold values from 0.1 to 1.9
- layer_weight: bfloat16 [4, 4096, 4096], P(None, None, 'col'), may hold values from -0.09375 to 0.09375
Outputs:
- packed_out: bfloat16 [1024, 4096], P('row', 'col')
The draws below stay inside these ranges and needn't reach their ends.
Inputs may be any that keep to these rules, and one draw needn't show every extreme that they name: `task_ids`: 8 marks an empty row, smaller values name a task.
All inputs are finite; a program needn't handle non-finite values.
Results may differ from the reference program's by a relative error of at most 0.008.
Values may be sent and summed in bfloat16 or wider, within the bound.
A program may use at most 128 MiB of HBM per device.

```python
import jax
import jax.numpy as jnp
from jax import lax

D = 4096
N_TASK = 8
LAYERS = 4
ROWS_DEV = 32
ROWS_TOTAL = 1024
N_ROW = 4
N_COL = 8


def draw_task_ids(key, part):
    first_key, second_key = jax.random.split(jax.random.fold_in(key, 11))
    device_count = N_ROW * N_COL
    live_rows = jax.random.randint(first_key, (device_count, 1), 3 * ROWS_DEV // 4, ROWS_DEV + 1)
    picked = jax.random.randint(second_key, (device_count, ROWS_DEV), 0, N_TASK)
    positions = jnp.arange(ROWS_DEV, dtype=jnp.int32)[None, :]
    table = jnp.where(positions < live_rows, picked, N_TASK)
    return table.reshape(-1).astype(jnp.int32)


def block_levels(rng, extent, cuts, least, largest):
    loudness = 1.0
    for position, blocks in cuts:
        draws = jax.random.uniform(jax.random.fold_in(jax.random.fold_in(rng, 6), position), (blocks,), jnp.float32, least / len(cuts), largest / len(cuts))
        loudness = loudness * jnp.repeat(jnp.exp(draws), extent[position] // blocks).reshape((-1,) + (1,) * (len(extent) - 1 - position))
    return loudness


def gaussian(key, extent, width, limit, shards=(), kind=jnp.bfloat16):
    drawn = jax.random.normal(key, extent, jnp.float32) * width
    if len(shards) > 0:
        drawn = block_levels(key, extent, shards, -0.22, 0.18) * drawn
    return jnp.clip(drawn, min=-limit, max=limit).astype(kind)


def setup_inputs(seed: int = 0) -> dict:
    streams_of = jax.random.split(jax.random.key(seed), 6)
    rows = gaussian(streams_of[0], (ROWS_TOTAL, D), 1.0, 6.0, ((0, 32),))
    task_ids = draw_task_ids(jax.random.fold_in(streams_of[5], 71), 0)
    task_embed = gaussian(streams_of[2], (N_TASK, D), 1.0, 6.0)
    norm_gain = jnp.clip(1.0 + 0.18 * jax.random.normal(streams_of[3], (LAYERS, D), jnp.float32), 0.1, 1.9)
    layer_weight = gaussian(streams_of[4], (LAYERS, D, D), D ** -0.5, 0.09375, ((2, 8),))
    return {"rows": rows, "task_ids": task_ids, "task_embed": task_embed, "norm_gain": norm_gain, "layer_weight": layer_weight}


epsilon = 1e-06

def reference(rows, task_ids, task_embed, norm_gain, layer_weight):
    device_count = N_ROW * N_COL
    row_total = device_count * ROWS_DEV
    task_table = task_ids.reshape(device_count, ROWS_DEV)
    task_range = jnp.arange(N_TASK, dtype=jnp.int32)
    member = (task_table[:, :, None] == task_range[None, None, :]).astype(jnp.int32)
    counts = lax.optimization_barrier(jnp.sum(member, axis=1)).astype(jnp.int32)
    before = (jnp.cumsum(counts, axis=0) - counts).astype(jnp.int32)
    totals = lax.optimization_barrier(jnp.sum(counts, axis=0)).astype(jnp.int32)
    task_base = (jnp.cumsum(totals) - totals).astype(jnp.int32)
    task_rank = lax.optimization_barrier(jnp.sum(member * (jnp.cumsum(member, axis=1) - member), axis=2)).astype(jnp.int32)
    packed_pos = (lax.optimization_barrier(jnp.sum(member * (task_base[None, None, :] + before[:, None, :]), axis=2)) + task_rank).astype(jnp.int32)
    target = jnp.where(task_table < N_TASK, packed_pos, row_total).reshape(-1).astype(jnp.int32)
    packed = jnp.zeros((row_total, D), jnp.bfloat16).at[target].set(rows, mode='drop')
    slot_pos = jnp.arange(row_total, dtype=jnp.int32)
    in_task = (slot_pos[:, None] >= task_base[None, :]) & (slot_pos[:, None] < (task_base + totals)[None, :])
    task_term = jnp.dot(in_task.astype(jnp.bfloat16), task_embed, preferred_element_type=jnp.float32)
    hidden = (packed.astype(jnp.float32) + task_term).astype(jnp.bfloat16)
    hidden = hidden.reshape(ROWS_DEV * N_COL, N_ROW, D).transpose(1, 0, 2).reshape(row_total, D)
    for layer_index in range(LAYERS):
        values = hidden.astype(jnp.float32)
        inverse_rms = lax.rsqrt(lax.optimization_barrier(jnp.mean(values * values, axis=1, keepdims=True)) + epsilon)
        active = jax.nn.silu(values * inverse_rms * norm_gain[layer_index][None, :]).astype(jnp.bfloat16)
        update = jnp.dot(active, layer_weight[layer_index], preferred_element_type=jnp.float32)
        hidden = (values + update).astype(jnp.bfloat16)
    return hidden
```

```python
import functools

import jax
import jax.numpy as jnp
from jax import lax
from jax.experimental import pallas as pl
from jax.experimental.pallas import tpu as pltpu
from jax.sharding import PartitionSpec as P

epsilon = 1e-06
MESH = pl.DeviceIdType.MESH
INNER = 2
CHUNKS = 4
SUB = 16
LEAD1 = 2
LEAD2 = 1
F32 = jnp.float32
BF16 = jnp.bfloat16


def kernel(
    sizes,
    rows_ref,
    ids_ref,
    embed_ref,
    gain_ref,
    weight_ref,
    out_ref,
    weight,
    hidden,
    active,
    gain,
    income,
    put,
    id_own,
    id_row,
    id_sum,
    id_col,
    sem_weight,
    send_idrow,
    recv_idrow,
    send_idcol,
    recv_idcol,
    send_row,
    recv_row,
    send_own,
    send_relay,
    send_along,
    recv_hidden,
):
    n_row, n_col, layers, chunks, tasks = sizes
    n_outer = n_col // INNER
    rows_dev = rows_ref.shape[0]
    width = rows_ref.shape[1]
    part = width // n_col
    slots = rows_dev * n_col
    m = slots // chunks
    steps = layers * chunks
    groups = rows_dev // SUB
    halves = chunks // groups
    span = n_col // halves
    me_r = lax.axis_index("row")
    me_c = lax.axis_index("col")
    outer = me_c // INNER
    inner = me_c % INNER
    partner = outer * INNER + (INNER - 1 - inner)

    def col_peer(j):
        return (me_c + j) % n_col

    def row_peer(j):
        return (me_r + j) % n_row

    def remote(src, dst, send, recv, r, c):
        return pltpu.make_async_remote_copy(
            src_ref=src, dst_ref=dst, send_sem=send, recv_sem=recv, device_id=(r, c), device_id_type=MESH
        )

    def weight_copy(l):
        return pltpu.make_async_copy(weight_ref.at[l], weight.at[l], sem_weight.at[l])

    barrier = pltpu.get_barrier_semaphore()
    for j in range(1, n_row):
        pl.semaphore_signal(barrier, inc=1, device_id=(row_peer(j), me_c), device_id_type=MESH)
    for j in range(1, n_col):
        pl.semaphore_signal(barrier, inc=1, device_id=(me_r, col_peer(j)), device_id_type=MESH)

    for l in range(layers):
        weight_copy(l).start()

    lead_dim = id_own.shape[0]
    lanes = id_own.shape[1]
    per_tile = lanes // rows_dev
    raw_ids = ids_ref[...]
    spread = lax.broadcasted_iota(jnp.int32, (rows_dev, lanes), 1) - lax.broadcasted_iota(
        jnp.int32, (rows_dev, lanes), 0
    )
    spread = jnp.where(spread == (me_c % per_tile) * rows_dev, 1.0, 0.0).astype(BF16)
    own_ids = jnp.broadcast_to(raw_ids.astype(F32), (lead_dim, rows_dev)).astype(BF16)
    row_ids = jnp.dot(own_ids, spread, preferred_element_type=F32).astype(jnp.int32)
    sub = lax.broadcasted_iota(jnp.int32, (lead_dim, lanes), 0)
    id_own[...] = jnp.where(sub == me_r, row_ids, 0)

    eye = jnp.where(
        lax.broadcasted_iota(jnp.int32, (rows_dev, rows_dev), 0)
        == lax.broadcasted_iota(jnp.int32, (rows_dev, rows_dev), 1),
        1.0,
        0.0,
    ).astype(BF16)
    tall_ids = lax.dot_general(eye, own_ids, (((1,), (1,)), ((), ())), preferred_element_type=F32)[:, 0:1]
    embed_on = [jnp.where(tall_ids == float(t), 1.0, 0.0) for t in range(tasks)]
    for g in range(groups):
        lines = slice(g * SUB, (g + 1) * SUB)
        for c in range(n_col):
            cols = slice(c * part, (c + 1) * part)
            term = jnp.zeros((SUB, part), F32)
            for t in range(tasks):
                term = term + embed_on[t][lines, :] * embed_ref[t : t + 1, cols].astype(F32)
            begin = (rows_ref[lines, cols].astype(F32) + term).astype(BF16)
            hidden[g * halves + c // span, me_c, (c % span) * SUB : (c % span + 1) * SUB, :] = begin

    pl.semaphore_wait(barrier, n_row + n_col - 2)

    def id_row_copy(j):
        return remote(id_own, id_row.at[me_r], send_idrow.at[j], recv_idrow.at[me_r], row_peer(j), me_c)

    def id_row_from(j):
        return remote(id_own, id_row.at[row_peer(j)], send_idrow.at[j], recv_idrow.at[row_peer(j)], row_peer(j), me_c)

    def id_col_copy(j):
        return remote(id_sum, id_col.at[me_c], send_idcol.at[j], recv_idcol.at[me_c], me_r, col_peer(j))

    def id_col_from(j):
        return remote(id_sum, id_col.at[col_peer(j)], send_idcol.at[j], recv_idcol.at[col_peer(j)], me_r, col_peer(j))

    def row_copy(ch, j):
        block = income.at[ch, me_r]
        return remote(block, block, send_row.at[ch, j], recv_row.at[ch, me_r], row_peer(j), me_c)

    def row_from(ch, j):
        block = income.at[ch, row_peer(j)]
        return remote(block, block, send_row.at[ch, j], recv_row.at[ch, row_peer(j)], row_peer(j), me_c)

    half = n_outer // 2
    side = outer // half
    is_gate = outer == half - 1 + side
    far_gate = (half - side) * INNER + inner

    def near(j, i):
        return (side * half + (outer % half + j) % half) * INNER + i

    def far(k, i):
        return ((1 - side) * half + k) * INNER + i

    other = INNER - 1 - inner

    def block_copy(s, source, send, peer):
        block = hidden.at[s, source]
        return remote(block, block, send, recv_hidden.at[s, source], me_r, peer)

    def await_block(s, source):
        block_copy(s, source, send_relay.at[0, source], partner).wait_recv()

    def own_copies(s):
        peers = [near(j, inner) for j in range(1, half)] + [far_gate, partner]
        return [block_copy(s, me_c, send_own.at[s % chunks, peer], peer) for peer in peers]

    def send_all(s):
        for copy in own_copies(s):
            copy.start()

    def drain_own(s):
        for copy in own_copies(s):
            copy.wait_send()

    def over(s, source):
        return block_copy(s, source, send_relay.at[s % chunks, source], partner)

    def along(s, source, j):
        return block_copy(s, source, send_along.at[s % chunks, source // INNER, j], near(j, inner))

    def pass_on(s, go, source, copies):
        if go:
            await_block(s, source)
        for copy in copies:
            if go:
                copy.start()
            else:
                copy.wait_send()

    def first_relay(s, go):
        @pl.when(is_gate)
        def _():
            for k in range(half):
                source = far(k, inner)
                pass_on(s, go, source, [along(s, source, j) for j in range(1, half)] + [over(s, source)])

        @pl.when(s % 2 == 0)
        def _():
            for j in range(1, half):
                pass_on(s, go, near(j, inner), [over(s, near(j, inner))])

        @pl.when(s % 2 == 1)
        def _():
            pass_on(s, go, partner, [along(s, partner, j) for j in range(1, half)])

    def second_relay(s, go):
        @pl.when(jnp.logical_not(is_gate))
        def _():
            for k in range(half):
                pass_on(s, go, far(k, inner), [over(s, far(k, inner))])

    def await_rest(s):
        @pl.when(s % 2 == 0)
        def _():
            await_block(s, partner)

        @pl.when(s % 2 == 1)
        def _():
            for j in range(1, half):
                await_block(s, near(j, inner))

        for j in range(1, half):
            await_block(s, near(j, other))
        for k in range(half):
            await_block(s, far(k, other))

    def relay(s, relay_of):
        @pl.when(s < steps)
        def _():
            @pl.when(s >= chunks)
            def _():
                relay_of(s - chunks, False)

            relay_of(s, True)

    for j in range(1, n_row):
        id_row_copy(j).start()
    for ch in range(chunks):
        send_all(ch)

    for l in range(layers):
        gain[l] = gain_ref[l : l + 1, :]
    out_ref[...] = jnp.zeros(out_ref.shape, BF16)
    ids_here = id_own[...]
    for j in range(1, n_row):
        id_row_from(j).wait_recv()
        ids_here = ids_here + id_row[row_peer(j)]
    id_sum[...] = ids_here
    id_col[me_c] = ids_here
    for j in range(1, n_col):
        id_col_copy(j).start()

    for s in range(LEAD1):
        first_relay(jnp.int32(s), True)
    for s in range(LEAD2):
        second_relay(jnp.int32(s), True)

    for j in range(1, n_col):
        id_col_from(j).wait_recv()
    tiles = []
    for tile in range(n_col // per_tile):
        joined = id_col[tile * per_tile]
        for c in range(tile * per_tile + 1, (tile + 1) * per_tile):
            joined = joined + id_col[c]
        tiles.append(joined)
    ids = jnp.concatenate(tiles, 1)

    bits = SUB.bit_length() - 1
    wide = (n_col * SUB).bit_length() - 1

    def origin(lane):
        group = lane >> wide
        source = (lane >> bits) & (n_col - 1)
        return source * rows_dev + group * SUB + (lane & (SUB - 1))

    low = lax.broadcasted_iota(jnp.int32, (slots, slots), 0)
    high = lax.broadcasted_iota(jnp.int32, (slots, slots), 1)
    shuffle = jnp.where(low == origin(high), 1.0, 0.0).astype(BF16)
    earlier = jnp.where(origin(low) < origin(high), 1.0, 0.0).astype(BF16)
    ids = jnp.dot(ids.astype(F32).astype(BF16), shuffle, preferred_element_type=F32).astype(jnp.int32)
    line = lax.broadcasted_iota(jnp.int32, (lead_dim, slots), 0)
    line_col = lax.broadcasted_iota(jnp.int32, (lead_dim, 1), 0)
    ids = jnp.where(line < n_row, ids, tasks)
    live = ids < tasks
    member = [jnp.where(ids == t, 1.0, 0.0) for t in range(tasks)]
    ranks = jnp.dot(jnp.concatenate(member, 0).astype(BF16), earlier, preferred_element_type=F32)
    base = jnp.zeros((1, 1), F32)
    position = jnp.zeros((lead_dim, slots), F32)
    for t in range(tasks):
        count = jnp.sum(member[t], axis=1, keepdims=True)
        offset = jnp.zeros((lead_dim, 1), F32) + base
        for r in range(n_row):
            here = count[r : r + 1, :]
            offset = offset + jnp.where(line_col > r, here, 0.0)
            base = base + here
        rank = ranks[t * lead_dim : (t + 1) * lead_dim, :]
        position = position + member[t] * (offset + rank)
    slot = jnp.floor((position + 0.5) * (1.0 / n_row))
    target = jnp.where(live, position - slot * n_row, -1.0).astype(jnp.int32)
    slot = jnp.where(target == me_r, slot.astype(jnp.int32), -1)
    slot_range = lax.broadcasted_iota(jnp.int32, (slots, n_row * m), 0)
    for ch in range(chunks):
        aimed = jnp.concatenate([slot[r : r + 1, ch * m : (ch + 1) * m] for r in range(n_row)], 1)
        put[ch] = jnp.where(slot_range == aimed, 1.0, 0.0).astype(BF16)

    def silu(values):
        half = 0.5 * values
        return (half + half * jnp.tanh(half)).astype(BF16)

    def opening(g, carry):
        for h in range(halves):
            s = g * halves + h
            relay(s + LEAD2, second_relay)
            relay(s + LEAD1, first_relay)

            @pl.when(s == 0)
            def _():
                weight_copy(0).wait()

            await_rest(s)
        for c in range(n_col):
            lines = slice(c * SUB, (c + 1) * SUB)

            def piece(p):
                return hidden[g * halves + p // span, c, (p % span) * SUB : (p % span + 1) * SUB, :].astype(F32)

            total = jnp.zeros((SUB, part), F32)
            for p in range(n_col):
                values = piece(p)
                total = total + values * values
            inverse = lax.rsqrt(jnp.sum(total, axis=1, keepdims=True) * (1.0 / width) + epsilon)
            for p in range(n_col):
                cols = slice(p * part, (p + 1) * part)
                active[lines, cols] = silu(piece(p) * inverse * gain[0, :, cols])
        update = jnp.dot(active[...], weight[0], preferred_element_type=F32)
        own_lines = pl.ds(pl.multiple_of((me_c % span) * SUB, SUB), SUB)
        for h in range(halves):
            drain_own(g * halves + h)
        for c in range(n_col):
            own = hidden[g * halves + me_c // span, c, own_lines, :].astype(F32)
            result = (own + update[c * SUB : (c + 1) * SUB, :]).astype(BF16)
            hidden[chunks + g * halves + c // span, me_c, (c % span) * SUB : (c % span + 1) * SUB, :] = result
        for h in range(halves):
            send_all(chunks + g * halves + h)
        return carry

    lax.fori_loop(0, groups, opening, 0)

    def place(ch):
        for j in range(1, n_row):
            row_from(ch, j).wait_recv()
        arrived = income[ch].reshape(n_row * m, part)
        placed = jnp.dot(put[ch], arrived, preferred_element_type=F32)
        out_ref[...] = (out_ref[...].astype(F32) + placed).astype(BF16)

    def step(s, carry):
        l = s // chunks
        ch = s % chunks
        relay(s + LEAD2, second_relay)
        relay(s + LEAD1, first_relay)

        @pl.when(ch == 0)
        def _():
            weight_copy(l).wait()

        await_rest(s)
        total = jnp.zeros((m, part), F32)
        for c in range(n_col):
            values = hidden[s, c].astype(F32)
            total = total + values * values
        mean = jnp.sum(total, axis=1, keepdims=True) * (1.0 / width)
        inverse = lax.rsqrt(mean + epsilon)
        for c in range(n_col):
            cols = slice(c * part, (c + 1) * part)
            active[:m, cols] = silu(hidden[s, c].astype(F32) * inverse * gain[l, :, cols])
        update = jnp.dot(active[:m, :], weight[l], preferred_element_type=F32)
        result = (hidden[s, me_c].astype(F32) + update).astype(BF16)

        drain_own(s)

        @pl.when(l < layers - 1)
        def _():
            hidden[s + chunks, me_c] = result
            send_all(s + chunks)

        @pl.when(l == layers - 1)
        def _():
            income[ch, me_r] = result
            for j in range(1, n_row):
                row_copy(ch, j).start()

            @pl.when(ch >= 1)
            def _():
                place(ch - 1)

        return carry

    lax.fori_loop(chunks, steps, step, 0)
    place(chunks - 1)

    for ch in range(chunks):
        first_relay(jnp.int32(steps - chunks + ch), False)
        second_relay(jnp.int32(steps - chunks + ch), False)
        for j in range(1, n_row):
            row_copy(ch, j).wait_send()
    for j in range(1, n_row):
        id_row_copy(j).wait_send()
    for j in range(1, n_col):
        id_col_copy(j).wait_send()


def shards(rows, task_ids, task_embed, norm_gain, layer_weight):
    rows_dev, width = rows.shape
    tasks = task_embed.shape[0]
    layers = layer_weight.shape[0]
    part = layer_weight.shape[2]
    n_row = lax.axis_size("row")
    n_col = lax.axis_size("col")
    slots = rows_dev * n_col
    chunks = CHUNKS
    m = slots // chunks
    lead_dim = -(-n_row // 8) * 8
    lanes = 128
    sizes = (n_row, n_col, layers, chunks, tasks)
    dma = pltpu.SemaphoreType.DMA
    vmem = pl.BlockSpec(memory_space=pltpu.VMEM)
    return pl.pallas_call(
        functools.partial(kernel, sizes),
        out_shape=jax.ShapeDtypeStruct((slots, part), BF16),
        in_specs=[vmem, vmem, vmem, vmem, pl.BlockSpec(memory_space=pl.ANY)],
        out_specs=vmem,
        scratch_shapes=[
            pltpu.VMEM((layers, width, part), BF16),
            pltpu.VMEM((layers * chunks, n_col, m, part), BF16),
            pltpu.VMEM((n_col * SUB, width), BF16),
            pltpu.VMEM((layers, 1, width), F32),
            pltpu.VMEM((chunks, n_row, m, part), BF16),
            pltpu.VMEM((chunks, slots, n_row * m), BF16),
            pltpu.VMEM((lead_dim, lanes), jnp.int32),
            pltpu.VMEM((n_row, lead_dim, lanes), jnp.int32),
            pltpu.VMEM((lead_dim, lanes), jnp.int32),
            pltpu.VMEM((n_col, lead_dim, lanes), jnp.int32),
            dma((layers,)),
            dma((n_row,)),
            dma((n_row,)),
            dma((n_col,)),
            dma((n_col,)),
            dma((chunks, n_row)),
            dma((chunks, n_row)),
            dma((chunks, n_col)),
            dma((chunks, n_col)),
            dma((chunks, n_col // INNER, max(1, n_col // INNER // 2))),
            dma((layers * chunks, n_col)),
        ],
        compiler_params=pltpu.CompilerParams(
            collective_id=0, has_side_effects=True, vmem_limit_bytes=60 * 1024 * 1024
        ),
    )(rows, task_ids.reshape(1, rows_dev), task_embed, norm_gain, layer_weight)


def solution(mesh):
    return jax.shard_map(
        shards,
        mesh=mesh,
        in_specs=(P(("row", "col"), None), P(("row", "col")), P(), P(), P(None, None, "col")),
        out_specs=P("row", "col"),
        check_vma=False,
    )
```

```python
import functools
import math

import jax
import jax.numpy as jnp
from jax import lax
from jax.experimental import pallas as pl
from jax.experimental.pallas import tpu as pltpu
from jax.sharding import PartitionSpec as P

epsilon = 1e-06
MESH = pl.DeviceIdType.MESH
INNER = 2
CHUNKS = 4
SUB = 16
SPARE = 10 * 2**20
LEAD1 = 2
LEAD2 = 1
F32 = jnp.float32
BF16 = jnp.bfloat16


def kernel(
    sizes,
    rows_hbm,
    ids_hbm,
    embed_hbm,
    gain_hbm,
    weight_ref,
    out_ref,
    rows_ref,
    ids_ref,
    embed_ref,
    gain,
    weight,
    hidden,
    active,
    income,
    put,
    id_own,
    id_row,
    id_sum,
    id_col,
    sem_input,
    sem_gain,
    sem_weight,
    send_idrow,
    recv_idrow,
    send_idcol,
    recv_idcol,
    send_row,
    recv_row,
    send_own,
    send_relay,
    send_along,
    recv_hidden,
):
    n_row, n_col, layers, chunks, tasks = sizes
    n_outer = n_col // INNER
    rows_dev = rows_ref.shape[0]
    width = rows_ref.shape[1]
    part = width // n_col
    slots = rows_dev * n_col
    m = slots // chunks
    steps = layers * chunks
    groups = rows_dev // SUB
    halves = chunks // groups
    span = n_col // halves
    me_r = lax.axis_index("row")
    me_c = lax.axis_index("col")
    outer = me_c // INNER
    inner = me_c % INNER
    partner = outer * INNER + (INNER - 1 - inner)

    def col_peer(j):
        return (me_c + j) % n_col

    def row_peer(j):
        return (me_r + j) % n_row

    def remote(src, dst, send, recv, r, c):
        return pltpu.make_async_remote_copy(
            src_ref=src, dst_ref=dst, send_sem=send, recv_sem=recv, device_id=(r, c), device_id_type=MESH
        )

    def weight_copy(l):
        return pltpu.make_async_copy(weight_ref.at[l], weight.at[l], sem_weight.at[l])

    barrier = pltpu.get_barrier_semaphore()
    for j in range(1, n_row):
        pl.semaphore_signal(barrier, inc=1, device_id=(row_peer(j), me_c), device_id_type=MESH)
    for j in range(1, n_col):
        pl.semaphore_signal(barrier, inc=1, device_id=(me_r, col_peer(j)), device_id_type=MESH)

    inputs = [
        pltpu.make_async_copy(source, dest, sem_input.at[i])
        for i, (source, dest) in enumerate(((rows_hbm, rows_ref), (embed_hbm, embed_ref), (ids_hbm, ids_ref)))
    ]
    for copy in inputs:
        copy.start()

    def gain_copy(l):
        return pltpu.make_async_copy(gain_hbm.at[pl.ds(l, 1)], gain.at[l], sem_gain.at[l])

    out_ref[...] = jnp.zeros(out_ref.shape, BF16)
    for copy in inputs:
        copy.wait()
    for l in range(layers):
        gain_copy(l).start()
        weight_copy(l).start()

    lead_dim = id_own.shape[0]
    lanes = id_own.shape[1]
    per_tile = lanes // rows_dev
    raw_ids = ids_ref[...]
    spread = lax.broadcasted_iota(jnp.int32, (rows_dev, lanes), 1) - lax.broadcasted_iota(
        jnp.int32, (rows_dev, lanes), 0
    )
    spread = jnp.where(spread == (me_c % per_tile) * rows_dev, 1.0, 0.0).astype(BF16)
    own_ids = jnp.broadcast_to(raw_ids.astype(F32), (lead_dim, rows_dev)).astype(BF16)
    row_ids = jnp.dot(own_ids, spread, preferred_element_type=F32).astype(jnp.int32)
    sub = lax.broadcasted_iota(jnp.int32, (lead_dim, lanes), 0)
    id_own[...] = jnp.where(sub == me_r, row_ids, 0)

    eye = jnp.where(
        lax.broadcasted_iota(jnp.int32, (rows_dev, rows_dev), 0)
        == lax.broadcasted_iota(jnp.int32, (rows_dev, rows_dev), 1),
        1.0,
        0.0,
    ).astype(BF16)
    tall_ids = lax.dot_general(eye, own_ids, (((1,), (1,)), ((), ())), preferred_element_type=F32)[:, 0:1]
    embed_on = [jnp.where(tall_ids == float(t), 1.0, 0.0) for t in range(tasks)]
    for g in range(groups):
        lines = slice(g * SUB, (g + 1) * SUB)
        for c in range(n_col):
            cols = slice(c * part, (c + 1) * part)
            term = jnp.zeros((SUB, part), F32)
            for t in range(tasks):
                term = term + embed_on[t][lines, :] * embed_ref[t : t + 1, cols].astype(F32)
            begin = (rows_ref[lines, cols].astype(F32) + term).astype(BF16)
            hidden[g * halves + c // span, me_c, (c % span) * SUB : (c % span + 1) * SUB, :] = begin

    pl.semaphore_wait(barrier, n_row + n_col - 2)

    def id_row_copy(j):
        return remote(id_own, id_row.at[me_r], send_idrow.at[j], recv_idrow.at[me_r], row_peer(j), me_c)

    def id_row_from(j):
        return remote(id_own, id_row.at[row_peer(j)], send_idrow.at[j], recv_idrow.at[row_peer(j)], row_peer(j), me_c)

    def id_col_copy(j):
        return remote(id_sum, id_col.at[me_c], send_idcol.at[j], recv_idcol.at[me_c], me_r, col_peer(j))

    def id_col_from(j):
        return remote(id_sum, id_col.at[col_peer(j)], send_idcol.at[j], recv_idcol.at[col_peer(j)], me_r, col_peer(j))

    def row_copy(ch, j):
        block = income.at[ch, me_r]
        return remote(block, block, send_row.at[ch, j], recv_row.at[ch, me_r], row_peer(j), me_c)

    def row_from(ch, j):
        block = income.at[ch, row_peer(j)]
        return remote(block, block, send_row.at[ch, j], recv_row.at[ch, row_peer(j)], row_peer(j), me_c)

    half = n_outer // 2
    side = outer // half
    is_gate = outer == half - 1 + side
    far_gate = (half - side) * INNER + inner

    def near(j, i):
        return (side * half + (outer % half + j) % half) * INNER + i

    def far(k, i):
        return ((1 - side) * half + k) * INNER + i

    other = INNER - 1 - inner

    def block_copy(s, source, send, peer):
        block = hidden.at[s, source]
        return remote(block, block, send, recv_hidden.at[s, source], me_r, peer)

    def await_block(s, source):
        block_copy(s, source, send_relay.at[0, source], partner).wait_recv()

    def own_copies(s):
        peers = [near(j, inner) for j in range(1, half)] + [far_gate, partner]
        return [block_copy(s, me_c, send_own.at[s % chunks, peer], peer) for peer in peers]

    def send_all(s):
        for copy in own_copies(s):
            copy.start()

    def drain_own(s):
        for copy in own_copies(s):
            copy.wait_send()

    def over(s, source):
        return block_copy(s, source, send_relay.at[s % chunks, source], partner)

    def along(s, source, j):
        return block_copy(s, source, send_along.at[s % chunks, source // INNER, j], near(j, inner))

    def pass_on(s, go, source, copies):
        if go:
            await_block(s, source)
        for copy in copies:
            if go:
                copy.start()
            else:
                copy.wait_send()

    def first_relay(s, go):
        @pl.when(is_gate)
        def _():
            for k in range(half):
                source = far(k, inner)
                pass_on(s, go, source, [along(s, source, j) for j in range(1, half)] + [over(s, source)])

        @pl.when(s % 2 == 0)
        def _():
            for j in range(1, half):
                pass_on(s, go, near(j, inner), [over(s, near(j, inner))])

        @pl.when(s % 2 == 1)
        def _():
            pass_on(s, go, partner, [along(s, partner, j) for j in range(1, half)])

    def second_relay(s, go):
        @pl.when(jnp.logical_not(is_gate))
        def _():
            for k in range(half):
                pass_on(s, go, far(k, inner), [over(s, far(k, inner))])

    def await_rest(s):
        @pl.when(s % 2 == 0)
        def _():
            await_block(s, partner)

        @pl.when(s % 2 == 1)
        def _():
            for j in range(1, half):
                await_block(s, near(j, inner))

        for j in range(1, half):
            await_block(s, near(j, other))
        for k in range(half):
            await_block(s, far(k, other))

    def relay(s, relay_of):
        @pl.when(s < steps)
        def _():
            @pl.when(s >= chunks)
            def _():
                relay_of(s - chunks, False)

            relay_of(s, True)

    for j in range(1, n_row):
        id_row_copy(j).start()
    for ch in range(chunks):
        send_all(ch)

    for s in range(LEAD1):
        first_relay(jnp.int32(s), True)
    for s in range(LEAD2):
        second_relay(jnp.int32(s), True)

    def pass_ids():
        ids_here = id_own[...]
        for j in range(1, n_row):
            id_row_from(j).wait_recv()
            ids_here = ids_here + id_row[row_peer(j)]
        id_sum[...] = ids_here
        id_col[me_c] = ids_here
        for j in range(1, n_col):
            id_col_copy(j).start()

    def find_places():
        for j in range(1, n_col):
            id_col_from(j).wait_recv()
        tiles = []
        for tile in range(n_col // per_tile):
            joined = id_col[tile * per_tile]
            for c in range(tile * per_tile + 1, (tile + 1) * per_tile):
                joined = joined + id_col[c]
            tiles.append(joined)
        ids = jnp.concatenate(tiles, 1)

        bits = SUB.bit_length() - 1
        wide = (n_col * SUB).bit_length() - 1

        def origin(lane):
            group = lane >> wide
            source = (lane >> bits) & (n_col - 1)
            return source * rows_dev + group * SUB + (lane & (SUB - 1))

        low = lax.broadcasted_iota(jnp.int32, (slots, slots), 0)
        high = lax.broadcasted_iota(jnp.int32, (slots, slots), 1)
        shuffle = jnp.where(low == origin(high), 1.0, 0.0).astype(BF16)
        earlier = jnp.where(origin(low) < origin(high), 1.0, 0.0).astype(BF16)
        ids = jnp.dot(ids.astype(F32).astype(BF16), shuffle, preferred_element_type=F32).astype(jnp.int32)
        line = lax.broadcasted_iota(jnp.int32, (lead_dim, slots), 0)
        line_col = lax.broadcasted_iota(jnp.int32, (lead_dim, 1), 0)
        ids = jnp.where(line < n_row, ids, tasks)
        live = ids < tasks
        member = [jnp.where(ids == t, 1.0, 0.0) for t in range(tasks)]
        ranks = jnp.dot(jnp.concatenate(member, 0).astype(BF16), earlier, preferred_element_type=F32)
        base = jnp.zeros((1, 1), F32)
        position = jnp.zeros((lead_dim, slots), F32)
        for t in range(tasks):
            count = jnp.sum(member[t], axis=1, keepdims=True)
            offset = jnp.zeros((lead_dim, 1), F32) + base
            for r in range(n_row):
                here = count[r : r + 1, :]
                offset = offset + jnp.where(line_col > r, here, 0.0)
                base = base + here
            rank = ranks[t * lead_dim : (t + 1) * lead_dim, :]
            position = position + member[t] * (offset + rank)
        slot = jnp.floor((position + 0.5) * (1.0 / n_row))
        target = jnp.where(live, position - slot * n_row, -1.0).astype(jnp.int32)
        slot = jnp.where(target == me_r, slot.astype(jnp.int32), -1)
        slot_range = lax.broadcasted_iota(jnp.int32, (slots, n_row * m), 0)
        for ch in range(chunks):
            aimed = jnp.concatenate([slot[r : r + 1, ch * m : (ch + 1) * m] for r in range(n_row)], 1)
            put[ch] = jnp.where(slot_range == aimed, 1.0, 0.0).astype(BF16)

    def silu(values):
        half = 0.5 * values
        return (half + half * jnp.tanh(half)).astype(BF16)

    def opening(g, carry):
        for h in range(halves):
            s = g * halves + h
            relay(s + LEAD2, second_relay)
            relay(s + LEAD1, first_relay)

            @pl.when(s == 0)
            def _():
                weight_copy(0).wait()
                for l in range(layers):
                    gain_copy(l).wait()

            await_rest(s)
        for c in range(n_col):
            lines = slice(c * SUB, (c + 1) * SUB)

            def piece(p):
                return hidden[g * halves + p // span, c, (p % span) * SUB : (p % span + 1) * SUB, :].astype(F32)

            total = jnp.zeros((SUB, part), F32)
            for p in range(n_col):
                values = piece(p)
                total = total + values * values
            inverse = lax.rsqrt(jnp.sum(total, axis=1, keepdims=True) * (1.0 / width) + epsilon)
            for p in range(n_col):
                cols = slice(p * part, (p + 1) * part)
                active[lines, cols] = silu(piece(p) * inverse * gain[0, :, cols])
        update = jnp.dot(active[...], weight[0], preferred_element_type=F32)
        own_lines = pl.ds(pl.multiple_of((me_c % span) * SUB, SUB), SUB)
        for h in range(halves):
            drain_own(g * halves + h)
        for c in range(n_col):
            own = hidden[g * halves + me_c // span, c, own_lines, :].astype(F32)
            result = (own + update[c * SUB : (c + 1) * SUB, :]).astype(BF16)
            hidden[chunks + g * halves + c // span, me_c, (c % span) * SUB : (c % span + 1) * SUB, :] = result
        for h in range(halves):
            send_all(chunks + g * halves + h)
        return carry

    lax.fori_loop(0, groups, opening, 0)

    def place(ch):
        for j in range(1, n_row):
            row_from(ch, j).wait_recv()
        arrived = income[ch].reshape(n_row * m, part)
        placed = jnp.dot(put[ch], arrived, preferred_element_type=F32)
        out_ref[...] = (out_ref[...].astype(F32) + placed).astype(BF16)

    def step(s, carry):
        l = s // chunks
        ch = s % chunks
        relay(s + LEAD2, second_relay)
        relay(s + LEAD1, first_relay)

        @pl.when(ch == 0)
        def _():
            weight_copy(l).wait()

        await_rest(s)
        total = jnp.zeros((m, part), F32)
        for c in range(n_col):
            values = hidden[s, c].astype(F32)
            total = total + values * values
        mean = jnp.sum(total, axis=1, keepdims=True) * (1.0 / width)
        inverse = lax.rsqrt(mean + epsilon)
        for c in range(n_col):
            cols = slice(c * part, (c + 1) * part)
            active[:m, cols] = silu(hidden[s, c].astype(F32) * inverse * gain[l, :, cols])
        update = jnp.dot(active[:m, :], weight[l], preferred_element_type=F32)
        result = (hidden[s, me_c].astype(F32) + update).astype(BF16)

        drain_own(s)

        @pl.when(l < layers - 1)
        def _():
            hidden[s + chunks, me_c] = result
            send_all(s + chunks)

        @pl.when(l == layers - 1)
        def _():
            income[ch, me_r] = result
            for j in range(1, n_row):
                row_copy(ch, j).start()

            @pl.when(ch >= 1)
            def _():
                place(ch - 1)

        @pl.when(s == chunks)
        def _():
            pass_ids()

        @pl.when(s == 2 * chunks)
        def _():
            find_places()

        return carry

    lax.fori_loop(chunks, steps, step, 0)
    for ch in range(chunks):
        first_relay(jnp.int32(steps - chunks + ch), False)
        second_relay(jnp.int32(steps - chunks + ch), False)
    for j in range(1, n_row):
        id_row_copy(j).wait_send()
    for j in range(1, n_col):
        id_col_copy(j).wait_send()
    for ch in range(chunks - 1):
        for j in range(1, n_row):
            row_copy(ch, j).wait_send()
    place(chunks - 1)
    for j in range(1, n_row):
        row_copy(chunks - 1, j).wait_send()


def shards(rows, task_ids, task_embed, norm_gain, layer_weight):
    rows_dev, width = rows.shape
    tasks = task_embed.shape[0]
    layers = layer_weight.shape[0]
    part = layer_weight.shape[2]
    n_row = lax.axis_size("row")
    n_col = lax.axis_size("col")
    slots = rows_dev * n_col
    chunks = CHUNKS
    m = slots // chunks
    lead_dim = -(-n_row // 8) * 8
    lanes = 128
    sizes = (n_row, n_col, layers, chunks, tasks)
    buffers = [
        pltpu.VMEM((rows_dev, width), BF16),
        pltpu.VMEM((1, rows_dev), jnp.int32),
        pltpu.VMEM((tasks, width), BF16),
        pltpu.VMEM((layers, 1, width), F32),
        pltpu.VMEM((layers, width, part), BF16),
        pltpu.VMEM((layers * chunks, n_col, m, part), BF16),
        pltpu.VMEM((n_col * SUB, width), BF16),
        pltpu.VMEM((chunks, n_row, m, part), BF16),
        pltpu.VMEM((chunks, slots, n_row * m), BF16),
        pltpu.VMEM((lead_dim, lanes), jnp.int32),
        pltpu.VMEM((n_row, lead_dim, lanes), jnp.int32),
        pltpu.VMEM((lead_dim, lanes), jnp.int32),
        pltpu.VMEM((n_col, lead_dim, lanes), jnp.int32),
    ]
    held = sum(math.prod(b.shape) * jnp.dtype(b.dtype).itemsize for b in buffers)
    dma = pltpu.SemaphoreType.DMA
    vmem = pl.BlockSpec(memory_space=pltpu.VMEM)
    hbm = pl.BlockSpec(memory_space=pltpu.HBM)
    operands = [rows, task_ids.reshape(1, rows_dev), task_embed, norm_gain, layer_weight]
    return pl.pallas_call(
        functools.partial(kernel, sizes),
        out_shape=jax.ShapeDtypeStruct((slots, part), BF16),
        in_specs=[hbm] * 5,
        out_specs=vmem,
        scratch_shapes=buffers
        + [
            dma((3,)),
            dma((layers,)),
            dma((layers,)),
            dma((n_row,)),
            dma((n_row,)),
            dma((n_col,)),
            dma((n_col,)),
            dma((chunks, n_row)),
            dma((chunks, n_row)),
            dma((chunks, n_col)),
            dma((chunks, n_col)),
            dma((chunks, n_col // INNER, max(1, n_col // INNER // 2))),
            dma((layers * chunks, n_col)),
        ],
        compiler_params=pltpu.CompilerParams(
            collective_id=0, has_side_effects=True, vmem_limit_bytes=min(held + SPARE, 60 * 2**20)
        ),
    )(*[pltpu.with_memory_space_constraint(operand, pltpu.HBM) for operand in operands])


def solution(mesh):
    return jax.shard_map(
        shards,
        mesh=mesh,
        in_specs=(P(("row", "col"), None), P(("row", "col")), P(), P(), P(None, None, "col")),
        out_specs=P("row", "col"),
        check_vma=False,
    )
```

```python
import functools
import math

import jax
import jax.numpy as jnp
from jax import lax
from jax.experimental import pallas as pl
from jax.experimental.pallas import tpu as pltpu
from jax.sharding import PartitionSpec as P

epsilon = 1e-06
MESH = pl.DeviceIdType.MESH
INNER = 2
CHUNKS = 4
SUB = 16
SPARE = 10 * 2**20
LEAD1 = 2
LEAD2 = 1
SHIP = {1: (0,), 4: (1,), 6: (2,), 8: (3,)}
SPREAD = {4: (0,), 6: (1,), 8: (2,), 10: (3,)}
RELAY = {5: (0,), 7: (1,), 9: (2,), 11: (3,)}
F32 = jnp.float32
BF16 = jnp.bfloat16


def kernel(
    sizes,
    rows_hbm,
    ids_hbm,
    embed_hbm,
    gain_hbm,
    weight_ref,
    out_ref,
    rows_ref,
    ids_ref,
    embed_ref,
    gain,
    weight,
    hidden,
    active,
    income,
    put,
    helped,
    part_out,
    part_in,
    scale_out,
    scale_in,
    id_own,
    id_row,
    id_sum,
    id_col,
    sem_input,
    sem_gain,
    sem_weight,
    send_idrow,
    recv_idrow,
    send_idcol,
    recv_idcol,
    send_row,
    recv_row,
    send_own,
    send_relay,
    send_along,
    recv_hidden,
    send_help,
    recv_help,
    send_part,
    recv_part,
    send_scale,
    recv_scale,
):
    n_row, n_col, layers, chunks, tasks, assisted = sizes
    n_outer = n_col // INNER
    rows_dev = rows_ref.shape[0]
    width = rows_ref.shape[1]
    part = width // n_col
    slots = rows_dev * n_col
    m = slots // chunks
    steps = layers * chunks
    first_helped = layers - assisted
    bound = first_helped * chunks
    groups = rows_dev // SUB
    halves = chunks // groups
    span = n_col // halves
    me_r = lax.axis_index("row")
    me_c = lax.axis_index("col")
    outer = me_c // INNER
    inner = me_c % INNER
    partner = outer * INNER + (INNER - 1 - inner)

    def columns(c):
        return pl.ds(pl.multiple_of(c * part, part), part)

    def col_peer(j):
        return (me_c + j) % n_col

    def row_peer(j):
        return (me_r + j) % n_row

    def remote(src, dst, send, recv, r, c):
        return pltpu.make_async_remote_copy(
            src_ref=src, dst_ref=dst, send_sem=send, recv_sem=recv, device_id=(r, c), device_id_type=MESH
        )

    def weight_copy(l):
        return pltpu.make_async_copy(weight_ref.at[l], weight.at[l], sem_weight.at[l])

    barrier = pltpu.get_barrier_semaphore()
    for j in range(1, n_row):
        pl.semaphore_signal(barrier, inc=1, device_id=(row_peer(j), me_c), device_id_type=MESH)
    for j in range(1, n_col):
        pl.semaphore_signal(barrier, inc=1, device_id=(me_r, col_peer(j)), device_id_type=MESH)

    inputs = [
        pltpu.make_async_copy(source, dest, sem_input.at[i])
        for i, (source, dest) in enumerate(((rows_hbm, rows_ref), (embed_hbm, embed_ref), (ids_hbm, ids_ref)))
    ]
    for copy in inputs:
        copy.start()

    def gain_copy(l):
        return pltpu.make_async_copy(gain_hbm.at[pl.ds(l, 1)], gain.at[l], sem_gain.at[l])

    out_ref[...] = jnp.zeros(out_ref.shape, BF16)
    for copy in inputs:
        copy.wait()
    for l in range(layers):
        gain_copy(l).start()
        weight_copy(l).start()

    lead_dim = id_own.shape[0]
    lanes = id_own.shape[1]
    per_tile = lanes // rows_dev
    raw_ids = ids_ref[...]
    spread = lax.broadcasted_iota(jnp.int32, (rows_dev, lanes), 1) - lax.broadcasted_iota(
        jnp.int32, (rows_dev, lanes), 0
    )
    spread = jnp.where(spread == (me_c % per_tile) * rows_dev, 1.0, 0.0).astype(BF16)
    own_ids = jnp.broadcast_to(raw_ids.astype(F32), (lead_dim, rows_dev)).astype(BF16)
    row_ids = jnp.dot(own_ids, spread, preferred_element_type=F32).astype(jnp.int32)
    sub = lax.broadcasted_iota(jnp.int32, (lead_dim, lanes), 0)
    id_own[...] = jnp.where(sub == me_r, row_ids, 0)

    eye = jnp.where(
        lax.broadcasted_iota(jnp.int32, (rows_dev, rows_dev), 0)
        == lax.broadcasted_iota(jnp.int32, (rows_dev, rows_dev), 1),
        1.0,
        0.0,
    ).astype(BF16)
    tall_ids = lax.dot_general(eye, own_ids, (((1,), (1,)), ((), ())), preferred_element_type=F32)[:, 0:1]
    embed_on = [jnp.where(tall_ids == float(t), 1.0, 0.0) for t in range(tasks)]
    for g in range(groups):
        lines = slice(g * SUB, (g + 1) * SUB)
        for c in range(n_col):
            cols = slice(c * part, (c + 1) * part)
            term = jnp.zeros((SUB, part), F32)
            for t in range(tasks):
                term = term + embed_on[t][lines, :] * embed_ref[t : t + 1, cols].astype(F32)
            begin = (rows_ref[lines, cols].astype(F32) + term).astype(BF16)
            hidden[g * halves + c // span, me_c, (c % span) * SUB : (c % span + 1) * SUB, :] = begin

    pl.semaphore_wait(barrier, n_row + n_col - 2)

    def id_row_copy(j):
        return remote(id_own, id_row.at[me_r], send_idrow.at[j], recv_idrow.at[me_r], row_peer(j), me_c)

    def id_row_from(j):
        return remote(id_own, id_row.at[row_peer(j)], send_idrow.at[j], recv_idrow.at[row_peer(j)], row_peer(j), me_c)

    def id_col_copy(j):
        return remote(id_sum, id_col.at[me_c], send_idcol.at[j], recv_idcol.at[me_c], me_r, col_peer(j))

    def id_col_from(j):
        return remote(id_sum, id_col.at[col_peer(j)], send_idcol.at[j], recv_idcol.at[col_peer(j)], me_r, col_peer(j))

    def row_copy(ch, j):
        block = income.at[ch, me_r]
        return remote(block, block, send_row.at[ch, j], recv_row.at[ch, me_r], row_peer(j), me_c)

    def row_from(ch, j):
        block = income.at[ch, row_peer(j)]
        return remote(block, block, send_row.at[ch, j], recv_row.at[ch, row_peer(j)], row_peer(j), me_c)

    half = n_outer // 2
    side = outer // half
    is_gate = outer == half - 1 + side
    far_gate = (half - side) * INNER + inner

    def near(j, i):
        return (side * half + (outer % half + j) % half) * INNER + i

    def far(k, i):
        return ((1 - side) * half + k) * INNER + i

    other = INNER - 1 - inner

    def block_copy(s, source, send, peer):
        block = hidden.at[s, source]
        return remote(block, block, send, recv_hidden.at[s, source], me_r, peer)

    def await_block(s, source):
        block_copy(s, source, send_relay.at[0, source], partner).wait_recv()

    def own_copies(s):
        peers = [near(j, inner) for j in range(1, half)] + [partner]
        return [block_copy(s, me_c, send_own.at[s % chunks, peer], peer) for peer in peers]

    def far_copy(s):
        return block_copy(s, me_c, send_own.at[s % chunks, far_gate], far_gate)

    def send_all(s):
        for copy in own_copies(s):
            copy.start()
        far_copy(s).start()

    def drain_own(s):
        for copy in own_copies(s):
            copy.wait_send()
        far_copy(s).wait_send()

    def over(s, source):
        return block_copy(s, source, send_relay.at[s % chunks, source], partner)

    def along(s, source, j):
        return block_copy(s, source, send_along.at[s % chunks, source // INNER, j], near(j, inner))

    def across(s, source):
        return block_copy(s, source, send_along.at[s % chunks, source // INNER, 0], far_gate)

    def pass_on(s, go, source, copies):
        if go:
            await_block(s, source)
        for copy in copies:
            if go:
                copy.start()
            else:
                copy.wait_send()

    mate = near(1, inner)
    far_corner = far(1 - side, inner) if half == 2 else far_gate
    even_of = lambda s: s % 2 == 0
    odd_of = lambda s: s % 2 == 1

    def full_first(s, go):
        @pl.when(is_gate)
        def _():
            for k in range(half):
                source = far(k, inner)
                pass_on(s, go, source, [along(s, source, j) for j in range(1, half)] + [over(s, source)])

        @pl.when(even_of(s))
        def _():
            for j in range(1, half):
                pass_on(s, go, near(j, inner), [over(s, near(j, inner))])

        @pl.when(odd_of(s))
        def _():
            pass_on(s, go, partner, [along(s, partner, j) for j in range(1, half)])

    def full_second(s, go):
        @pl.when(jnp.logical_not(is_gate))
        def _():
            for k in range(half):
                pass_on(s, go, far(k, inner), [over(s, far(k, inner))])

    def helped_first(s, go):
        @pl.when(jnp.logical_not(is_gate))
        def _():
            pass_on(s, go, partner, [along(s, partner, 1)])
            pass_on(s, go, mate, [over(s, mate)])

        @pl.when(is_gate & odd_of(s))
        def _():
            pass_on(s, go, partner, [across(s, partner)])

    def helped_second(s, go):
        @pl.when(is_gate & even_of(s))
        def _():
            pass_on(s, go, far_gate, [over(s, far_gate)])

        @pl.when(is_gate)
        def _():
            pass_on(s, go, far_corner, [over(s, far_corner)])

    def either(s, full, helped_one, go):
        if not assisted:
            full(s, go)
            return

        @pl.when(s < bound)
        def _():
            full(s, go)

        @pl.when(s >= bound)
        def _():
            helped_one(s, go)

    def first_relay(s, go):
        either(s, full_first, helped_first, go)

    def second_relay(s, go):
        either(s, full_second, helped_second, go)

    def await_rest(s):
        @pl.when(even_of(s))
        def _():
            await_block(s, partner)

        @pl.when(odd_of(s))
        def _():
            for j in range(1, half):
                await_block(s, near(j, inner))

        for j in range(1, half):
            await_block(s, near(j, other))
        for k in range(half):
            await_block(s, far(k, other))

    def await_helped(s):
        @pl.when(is_gate & even_of(s))
        def _():
            await_block(s, partner)

        @pl.when(is_gate & odd_of(s))
        def _():
            await_block(s, far_gate)

        await_block(s, near(1, other))

        @pl.when(is_gate)
        def _():
            await_block(s, mate)
            for k in range(half):
                await_block(s, far(k, other))

    far_base = (1 - side) * (width // 2)
    near_base = side * (width // 2)
    share = width // 2 // n_row
    bite = share // chunks
    sibling = me_r + 1 - 2 * (me_r % 2)
    cross = (me_r + 2) % n_row

    def helped_part(i, q):
        return helped.at[i // chunks, q, pl.ds((i % chunks) * bite, bite), :]

    def ship_copy(i):
        lines = pl.ds(pl.multiple_of(far_base + me_r * share + (i % chunks) * bite, bite), bite)
        source = weight.at[first_helped + i // chunks, lines, :]
        return remote(source, helped_part(i, me_r), send_help.at[i, 0], recv_help.at[i, me_r], me_r, mate)

    def help_copy(i, q, way, peer):
        block = helped_part(i, q)
        return remote(block, block, send_help.at[i, way], recv_help.at[i, q], peer, me_c)

    def spread_copies(i):
        return [help_copy(i, me_r, 1, sibling), help_copy(i, me_r, 2, cross)]

    def part_copy(s):
        slot = s - bound
        return remote(
            part_out.at[s % chunks], part_in.at[slot], send_part.at[s % chunks], recv_part.at[slot], me_r, mate
        )

    def scale_copy(s):
        slot = s - bound
        return remote(
            scale_out.at[s % chunks], scale_in.at[slot], send_scale.at[s % chunks], recv_scale.at[slot], me_r, mate
        )

    def at_steps(s, table, action):
        for when, items in table.items():
            @pl.when(s == when)
            def _():
                for i in items:
                    action(i)

    def spread(i):
        help_copy(i, me_r, 1, sibling).wait_recv()
        for copy in spread_copies(i):
            copy.start()

    def pass_cross(i):
        help_copy(i, cross, 3, sibling).wait_recv()
        help_copy(i, cross, 3, sibling).start()

    def move_weights(s):
        @pl.when(is_gate)
        def _():
            at_steps(s, RELAY, pass_cross)
            at_steps(s, SPREAD, spread)

        @pl.when(jnp.logical_not(is_gate))
        def _():
            at_steps(s, SHIP, lambda i: ship_copy(i).start())

    def await_weights(l):
        for i in range(assisted * chunks):
            @pl.when(is_gate & (l == first_helped + i // chunks))
            def _():
                for q in (sibling, (cross + 1 - 2 * (me_r % 2))):
                    help_copy(i, q, 1, sibling).wait_recv()

    def drain_weights():
        for i in range(assisted * chunks):
            @pl.when(is_gate)
            def _():
                for copy in spread_copies(i) + [help_copy(i, cross, 3, sibling)]:
                    copy.wait_send()

            @pl.when(jnp.logical_not(is_gate))
            def _():
                ship_copy(i).wait_send()

    def relay(s, relay_of):
        @pl.when(s < steps)
        def _():
            @pl.when(s >= chunks)
            def _():
                relay_of(s - chunks, False)

            relay_of(s, True)

    for j in range(1, n_row):
        id_row_copy(j).start()
    for ch in range(chunks):
        send_all(ch)

    for s in range(LEAD1):
        first_relay(jnp.int32(s), True)
    for s in range(LEAD2):
        second_relay(jnp.int32(s), True)

    def pass_ids():
        ids_here = id_own[...]
        for j in range(1, n_row):
            id_row_from(j).wait_recv()
            ids_here = ids_here + id_row[row_peer(j)]
        id_sum[...] = ids_here
        id_col[me_c] = ids_here
        for j in range(1, n_col):
            id_col_copy(j).start()

    def find_places():
        for j in range(1, n_col):
            id_col_from(j).wait_recv()
        tiles = []
        for tile in range(n_col // per_tile):
            joined = id_col[tile * per_tile]
            for c in range(tile * per_tile + 1, (tile + 1) * per_tile):
                joined = joined + id_col[c]
            tiles.append(joined)
        ids = jnp.concatenate(tiles, 1)

        bits = SUB.bit_length() - 1
        wide = (n_col * SUB).bit_length() - 1

        def origin(lane):
            group = lane >> wide
            source = (lane >> bits) & (n_col - 1)
            return source * rows_dev + group * SUB + (lane & (SUB - 1))

        low = lax.broadcasted_iota(jnp.int32, (slots, slots), 0)
        high = lax.broadcasted_iota(jnp.int32, (slots, slots), 1)
        shuffle = jnp.where(low == origin(high), 1.0, 0.0).astype(BF16)
        earlier = jnp.where(origin(low) < origin(high), 1.0, 0.0).astype(BF16)
        ids = jnp.dot(ids.astype(F32).astype(BF16), shuffle, preferred_element_type=F32).astype(jnp.int32)
        line = lax.broadcasted_iota(jnp.int32, (lead_dim, slots), 0)
        line_col = lax.broadcasted_iota(jnp.int32, (lead_dim, 1), 0)
        ids = jnp.where(line < n_row, ids, tasks)
        live = ids < tasks
        member = [jnp.where(ids == t, 1.0, 0.0) for t in range(tasks)]
        ranks = jnp.dot(jnp.concatenate(member, 0).astype(BF16), earlier, preferred_element_type=F32)
        base = jnp.zeros((1, 1), F32)
        position = jnp.zeros((lead_dim, slots), F32)
        for t in range(tasks):
            count = jnp.sum(member[t], axis=1, keepdims=True)
            offset = jnp.zeros((lead_dim, 1), F32) + base
            for r in range(n_row):
                here = count[r : r + 1, :]
                offset = offset + jnp.where(line_col > r, here, 0.0)
                base = base + here
            rank = ranks[t * lead_dim : (t + 1) * lead_dim, :]
            position = position + member[t] * (offset + rank)
        slot = jnp.floor((position + 0.5) * (1.0 / n_row))
        target = jnp.where(live, position - slot * n_row, -1.0).astype(jnp.int32)
        slot = jnp.where(target == me_r, slot.astype(jnp.int32), -1)
        slot_range = lax.broadcasted_iota(jnp.int32, (slots, n_row * m), 0)
        for ch in range(chunks):
            aimed = jnp.concatenate([slot[r : r + 1, ch * m : (ch + 1) * m] for r in range(n_row)], 1)
            put[ch] = jnp.where(slot_range == aimed, 1.0, 0.0).astype(BF16)

    def silu(values):
        half = 0.5 * values
        return (half + half * jnp.tanh(half)).astype(BF16)

    def opening(g, carry):
        if assisted:
            @pl.when(g == 0)
            def _():
                for l in range(first_helped, layers):
                    weight_copy(l).wait()

            @pl.when(jnp.logical_not(is_gate))
            def _():
                at_steps(g, {g: SHIP[g] for g in SHIP if g < groups}, lambda i: ship_copy(i).start())

        @pl.when(g == 0)
        def _():
            for s in range(LEAD1, chunks):
                first_relay(jnp.int32(s), True)
            weight_copy(0).wait()
            for l in range(layers):
                gain_copy(l).wait()

        for h in range(halves):
            if h > 0:
                second_relay(g * halves + h, True)
            else:
                @pl.when(g > 0)
                def _():
                    second_relay(g * halves, True)
        for h in range(halves):
            await_rest(g * halves + h)
        for c in range(n_col):
            lines = slice(c * SUB, (c + 1) * SUB)

            def piece(p):
                return hidden[g * halves + p // span, c, (p % span) * SUB : (p % span + 1) * SUB, :].astype(F32)

            total = jnp.zeros((SUB, part), F32)
            for p in range(n_col):
                values = piece(p)
                total = total + values * values
            inverse = lax.rsqrt(jnp.sum(total, axis=1, keepdims=True) * (1.0 / width) + epsilon)
            for p in range(n_col):
                cols = slice(p * part, (p + 1) * part)
                active[lines, cols] = silu(piece(p) * inverse * gain[0, :, cols])
        update = jnp.dot(active[...], weight[0], preferred_element_type=F32)
        own_lines = pl.ds(pl.multiple_of((me_c % span) * SUB, SUB), SUB)
        for h in range(halves):
            drain_own(g * halves + h)
        for c in range(n_col):
            own = hidden[g * halves + me_c // span, c, own_lines, :].astype(F32)
            result = (own + update[c * SUB : (c + 1) * SUB, :]).astype(BF16)
            hidden[chunks + g * halves + c // span, me_c, (c % span) * SUB : (c % span + 1) * SUB, :] = result
        for h in range(halves):
            send_all(chunks + g * halves + h)
        if assisted:
            @pl.when(is_gate)
            def _():
                at_steps(g, {g: SPREAD[g] for g in SPREAD if g < groups}, spread)

        return carry

    lax.fori_loop(0, groups, opening, 0)
    for s in range(LEAD1):
        relay(jnp.int32(chunks + s), first_relay)
    for s in range(LEAD2):
        relay(jnp.int32(chunks + s), second_relay)

    def place(ch):
        for j in range(1, n_row):
            row_from(ch, j).wait_recv()
        arrived = income[ch].reshape(n_row * m, part)
        placed = jnp.dot(put[ch], arrived, preferred_element_type=F32)
        out_ref[...] = (out_ref[...].astype(F32) + placed).astype(BF16)

    def finish(s, l, ch, result):
        drain_own(s)

        @pl.when(l < layers - 1)
        def _():
            hidden[s + chunks, me_c] = result
            send_all(s + chunks)

        @pl.when(l == layers - 1)
        def _():
            income[ch, me_r] = result
            for j in range(1, n_row):
                row_copy(ch, j).start()

    def after(s, l, ch):
        @pl.when((l == layers - 1) & (ch >= 1))
        def _():
            place(ch - 1)

        @pl.when(s == chunks)
        def _():
            pass_ids()

        @pl.when(s == 2 * chunks)
        def _():
            find_places()

    def step(s, carry):
        l = s // chunks
        ch = s % chunks
        relay(s + LEAD2, second_relay)
        relay(s + LEAD1, first_relay)

        @pl.when((ch == 0) & (l < first_helped) if assisted else ch == 0)
        def _():
            weight_copy(l).wait()

        await_rest(s)
        total = jnp.zeros((m, part), F32)
        for c in range(n_col):
            values = hidden[s, c].astype(F32)
            total = total + values * values
        mean = jnp.sum(total, axis=1, keepdims=True) * (1.0 / width)
        inverse = lax.rsqrt(mean + epsilon)
        for c in range(n_col):
            cols = slice(c * part, (c + 1) * part)
            active[:m, cols] = silu(hidden[s, c].astype(F32) * inverse * gain[l, :, cols])
        update = jnp.dot(active[:m, :], weight[l], preferred_element_type=F32)
        result = (hidden[s, me_c].astype(F32) + update).astype(BF16)
        finish(s, l, ch, result)
        if assisted:
            move_weights(s)
        after(s, l, ch)
        return carry

    near_cols = pl.ds(pl.multiple_of(near_base, width // 2), width // 2)
    far_cols = pl.ds(pl.multiple_of(far_base, width // 2), width // 2)

    def activate(s, l, begin, inverse):
        for q in range(n_col // 2):
            c = begin * (n_col // 2) + q
            cols = columns(c)
            active[:m, cols] = silu(hidden[s, c].astype(F32) * inverse * gain[l, :, cols])

    def helped_step(s, carry):
        l = s // chunks
        ch = s % chunks
        square = lax.broadcasted_iota(jnp.int32, (m, m), 0) == lax.broadcasted_iota(jnp.int32, (m, m), 1)
        relay(s + LEAD2, second_relay)
        relay(s + LEAD1, first_relay)

        @pl.when(ch == 0)
        def _():
            await_weights(l)

        await_helped(s)

        @pl.when(is_gate)
        def _():
            total = jnp.zeros((m, part), F32)
            for c in range(n_col):
                values = hidden[s, c].astype(F32)
                total = total + values * values
            mean = jnp.sum(total, axis=1, keepdims=True) * (1.0 / width)
            inverse = lax.rsqrt(mean + epsilon)

            @pl.when(s >= bound + chunks)
            def _():
                scale_copy(s - chunks).wait_send()
                part_copy(s - chunks).wait_send()

            scale_out[ch, 0:1, 0:m] = jnp.sum(jnp.where(square, inverse, 0.0), axis=0, keepdims=True)
            scale_copy(s).start()
            activate(s, l, 1 - side, inverse)
            theirs = helped[l - first_helped].reshape(width // 2, part)
            part_out[ch] = jnp.dot(active[:m, far_cols], theirs, preferred_element_type=F32).astype(BF16)
            part_copy(s).start()
            activate(s, l, side, inverse)
            update = jnp.dot(active[:m, :], weight[l], preferred_element_type=F32)
            finish(s, l, ch, (hidden[s, me_c].astype(F32) + update).astype(BF16))

        @pl.when(jnp.logical_not(is_gate))
        def _():
            scale_copy(s).wait_recv()
            inverse = jnp.sum(jnp.where(square, scale_in[s - bound, 0:1, 0:m], 0.0), axis=1, keepdims=True)
            activate(s, l, side, inverse)
            update = jnp.dot(active[:m, near_cols], weight[l, near_cols, :], preferred_element_type=F32)
            part_copy(s).wait_recv()
            update = update + part_in[s - bound].astype(F32)
            finish(s, l, ch, (hidden[s, me_c].astype(F32) + update).astype(BF16))

        @pl.when(s == steps - 2)
        def _():
            drain_weights()

        after(s, l, ch)
        return carry

    lax.fori_loop(chunks, bound, step, 0)
    if assisted:
        lax.fori_loop(bound, steps, helped_step, 0)
    for ch in range(chunks):
        first_relay(jnp.int32(steps - chunks + ch), False)
        second_relay(jnp.int32(steps - chunks + ch), False)
    for j in range(1, n_row):
        id_row_copy(j).wait_send()
    for j in range(1, n_col):
        id_col_copy(j).wait_send()
    if assisted:
        @pl.when(is_gate)
        def _():
            for ch in range(chunks):
                scale_copy(steps - chunks + ch).wait_send()
                part_copy(steps - chunks + ch).wait_send()

    for ch in range(chunks - 1):
        for j in range(1, n_row):
            row_copy(ch, j).wait_send()
    place(chunks - 1)
    for j in range(1, n_row):
        row_copy(chunks - 1, j).wait_send()


def shards(rows, task_ids, task_embed, norm_gain, layer_weight):
    rows_dev, width = rows.shape
    tasks = task_embed.shape[0]
    layers = layer_weight.shape[0]
    part = layer_weight.shape[2]
    n_row = lax.axis_size("row")
    n_col = lax.axis_size("col")
    slots = rows_dev * n_col
    chunks = CHUNKS
    m = slots // chunks
    lead_dim = -(-n_row // 8) * 8
    lanes = 128
    assisted = 1 if n_col // INNER == 4 and n_row == 4 and chunks == 4 and layers >= 4 and m <= 128 else 0
    sizes = (n_row, n_col, layers, chunks, tasks, assisted)
    spots = max(assisted * chunks, 1)
    buffers = [
        pltpu.VMEM((rows_dev, width), BF16),
        pltpu.VMEM((1, rows_dev), jnp.int32),
        pltpu.VMEM((tasks, width), BF16),
        pltpu.VMEM((layers, 1, width), F32),
        pltpu.VMEM((layers, width, part), BF16),
        pltpu.VMEM((layers * chunks, n_col, m, part), BF16),
        pltpu.VMEM((n_col * SUB, width), BF16),
        pltpu.VMEM((chunks, n_row, m, part), BF16),
        pltpu.VMEM((chunks, slots, n_row * m), BF16),
        pltpu.VMEM((max(assisted, 1), n_row, width // 2 // n_row if assisted else 16, part), BF16),
        pltpu.VMEM((chunks, m, part), BF16),
        pltpu.VMEM((spots, m, part), BF16),
        pltpu.VMEM((chunks, 8, lanes), F32),
        pltpu.VMEM((spots, 8, lanes), F32),
        pltpu.VMEM((lead_dim, lanes), jnp.int32),
        pltpu.VMEM((n_row, lead_dim, lanes), jnp.int32),
        pltpu.VMEM((lead_dim, lanes), jnp.int32),
        pltpu.VMEM((n_col, lead_dim, lanes), jnp.int32),
    ]
    held = sum(math.prod(b.shape) * jnp.dtype(b.dtype).itemsize for b in buffers)
    dma = pltpu.SemaphoreType.DMA
    vmem = pl.BlockSpec(memory_space=pltpu.VMEM)
    hbm = pl.BlockSpec(memory_space=pltpu.HBM)
    operands = [rows, task_ids.reshape(1, rows_dev), task_embed, norm_gain, layer_weight]
    return pl.pallas_call(
        functools.partial(kernel, sizes),
        out_shape=jax.ShapeDtypeStruct((slots, part), BF16),
        in_specs=[hbm] * 5,
        out_specs=vmem,
        scratch_shapes=buffers
        + [
            dma((3,)),
            dma((layers,)),
            dma((layers,)),
            dma((n_row,)),
            dma((n_row,)),
            dma((n_col,)),
            dma((n_col,)),
            dma((chunks, n_row)),
            dma((chunks, n_row)),
            dma((chunks, n_col)),
            dma((chunks, n_col)),
            dma((chunks, n_col // INNER, max(1, n_col // INNER // 2))),
            dma((layers * chunks, n_col)),
            dma((spots, 4)),
            dma((spots, n_row)),
            dma((chunks,)),
            dma((spots,)),
            dma((chunks,)),
            dma((spots,)),
        ],
        compiler_params=pltpu.CompilerParams(
            collective_id=0, has_side_effects=True, vmem_limit_bytes=min(held + SPARE, 60 * 2**20)
        ),
    )(*[pltpu.with_memory_space_constraint(operand, pltpu.HBM) for operand in operands])


def solution(mesh):
    return jax.shard_map(
        shards,
        mesh=mesh,
        in_specs=(P(("row", "col"), None), P(("row", "col")), P(), P(), P(None, None, "col")),
        out_specs=P("row", "col"),
        check_vma=False,
    )
```

```python
import functools
import math

import jax
import jax.numpy as jnp
from jax import lax
from jax.experimental import pallas as pl
from jax.experimental.pallas import tpu as pltpu
from jax.sharding import PartitionSpec as P

epsilon = 1e-06
MESH = pl.DeviceIdType.MESH
INNER = 2
CHUNKS = 4
SUB = 16
SPARE = 10 * 2**20
LEAD1 = 2
LEAD2 = 1
SHIP = {0: (0,), 1: (1,), 5: (2,), 8: (3,)}
SPREAD = {1: (0,), 4: (1,), 7: (2,), 9: (3,)}
RELAY = {5: (0,), 6: (1,), 9: (2,), 11: (3,)}
F32 = jnp.float32
BF16 = jnp.bfloat16


def kernel(
    sizes,
    rows_hbm,
    ids_hbm,
    embed_hbm,
    gain_hbm,
    weight_ref,
    out_ref,
    rows_ref,
    ids_ref,
    embed_ref,
    gain,
    weight,
    hidden,
    active,
    income,
    put,
    helped,
    part_out,
    part_in,
    scale_out,
    scale_in,
    id_own,
    id_row,
    id_sum,
    id_col,
    sem_input,
    sem_gain,
    sem_weight,
    send_idrow,
    recv_idrow,
    send_idcol,
    recv_idcol,
    send_row,
    recv_row,
    send_own,
    send_relay,
    send_along,
    recv_hidden,
    send_help,
    recv_help,
    send_part,
    recv_part,
    send_scale,
    recv_scale,
):
    n_row, n_col, layers, chunks, tasks, assisted = sizes
    n_outer = n_col // INNER
    rows_dev = rows_ref.shape[0]
    width = rows_ref.shape[1]
    part = width // n_col
    slots = rows_dev * n_col
    m = slots // chunks
    steps = layers * chunks
    first_helped = layers - assisted
    bound = first_helped * chunks
    groups = rows_dev // SUB
    halves = chunks // groups
    span = n_col // halves
    me_r = lax.axis_index("row")
    me_c = lax.axis_index("col")
    outer = me_c // INNER
    inner = me_c % INNER
    partner = outer * INNER + (INNER - 1 - inner)

    def columns(c):
        return pl.ds(pl.multiple_of(c * part, part), part)

    def col_peer(j):
        return (me_c + j) % n_col

    def row_peer(j):
        return (me_r + j) % n_row

    def remote(src, dst, send, recv, r, c):
        return pltpu.make_async_remote_copy(
            src_ref=src, dst_ref=dst, send_sem=send, recv_sem=recv, device_id=(r, c), device_id_type=MESH
        )

    def weight_copy(l):
        return pltpu.make_async_copy(weight_ref.at[l], weight.at[l], sem_weight.at[l])

    barrier = pltpu.get_barrier_semaphore()
    for j in range(1, n_row):
        pl.semaphore_signal(barrier, inc=1, device_id=(row_peer(j), me_c), device_id_type=MESH)
    for j in range(1, n_col):
        pl.semaphore_signal(barrier, inc=1, device_id=(me_r, col_peer(j)), device_id_type=MESH)

    inputs = [
        pltpu.make_async_copy(source, dest, sem_input.at[i])
        for i, (source, dest) in enumerate(((rows_hbm, rows_ref), (embed_hbm, embed_ref), (ids_hbm, ids_ref)))
    ]
    for copy in inputs:
        copy.start()

    def gain_copy(l):
        return pltpu.make_async_copy(gain_hbm.at[pl.ds(l, 1)], gain.at[l], sem_gain.at[l])

    out_ref[...] = jnp.zeros(out_ref.shape, BF16)
    for copy in inputs:
        copy.wait()
    for l in range(layers):
        gain_copy(l).start()
        weight_copy(l).start()

    lead_dim = id_own.shape[0]
    lanes = id_own.shape[1]
    per_tile = lanes // rows_dev
    raw_ids = ids_ref[...]
    spread = lax.broadcasted_iota(jnp.int32, (rows_dev, lanes), 1) - lax.broadcasted_iota(
        jnp.int32, (rows_dev, lanes), 0
    )
    spread = jnp.where(spread == (me_c % per_tile) * rows_dev, 1.0, 0.0).astype(BF16)
    own_ids = jnp.broadcast_to(raw_ids.astype(F32), (lead_dim, rows_dev)).astype(BF16)
    row_ids = jnp.dot(own_ids, spread, preferred_element_type=F32).astype(jnp.int32)
    sub = lax.broadcasted_iota(jnp.int32, (lead_dim, lanes), 0)
    id_own[...] = jnp.where(sub == me_r, row_ids, 0)

    eye = jnp.where(
        lax.broadcasted_iota(jnp.int32, (rows_dev, rows_dev), 0)
        == lax.broadcasted_iota(jnp.int32, (rows_dev, rows_dev), 1),
        1.0,
        0.0,
    ).astype(BF16)
    tall_ids = lax.dot_general(eye, own_ids, (((1,), (1,)), ((), ())), preferred_element_type=F32)[:, 0:1]
    embed_on = [jnp.where(tall_ids == float(t), 1.0, 0.0) for t in range(tasks)]
    for g in range(groups):
        lines = slice(g * SUB, (g + 1) * SUB)
        for c in range(n_col):
            cols = slice(c * part, (c + 1) * part)
            term = jnp.zeros((SUB, part), F32)
            for t in range(tasks):
                term = term + embed_on[t][lines, :] * embed_ref[t : t + 1, cols].astype(F32)
            begin = (rows_ref[lines, cols].astype(F32) + term).astype(BF16)
            hidden[g * halves + c // span, me_c, (c % span) * SUB : (c % span + 1) * SUB, :] = begin

    pl.semaphore_wait(barrier, n_row + n_col - 2)

    def id_row_copy(j):
        return remote(id_own, id_row.at[me_r], send_idrow.at[j], recv_idrow.at[me_r], row_peer(j), me_c)

    def id_row_from(j):
        return remote(id_own, id_row.at[row_peer(j)], send_idrow.at[j], recv_idrow.at[row_peer(j)], row_peer(j), me_c)

    def id_col_copy(j):
        return remote(id_sum, id_col.at[me_c], send_idcol.at[j], recv_idcol.at[me_c], me_r, col_peer(j))

    def id_col_from(j):
        return remote(id_sum, id_col.at[col_peer(j)], send_idcol.at[j], recv_idcol.at[col_peer(j)], me_r, col_peer(j))

    def row_copy(ch, j):
        block = income.at[ch, me_r]
        return remote(block, block, send_row.at[ch, j], recv_row.at[ch, me_r], row_peer(j), me_c)

    def row_from(ch, j):
        block = income.at[ch, row_peer(j)]
        return remote(block, block, send_row.at[ch, j], recv_row.at[ch, row_peer(j)], row_peer(j), me_c)

    half = n_outer // 2
    side = outer // half
    is_gate = outer == half - 1 + side
    far_gate = (half - side) * INNER + inner

    def near(j, i):
        return (side * half + (outer % half + j) % half) * INNER + i

    def far(k, i):
        return ((1 - side) * half + k) * INNER + i

    other = INNER - 1 - inner

    def block_copy(s, source, send, peer):
        block = hidden.at[s, source]
        return remote(block, block, send, recv_hidden.at[s % (2 * chunks), source], me_r, peer)

    def await_block(s, source):
        block_copy(s, source, send_relay.at[0, 0], partner).wait_recv()

    def near_copies(s):
        return [block_copy(s, me_c, send_own.at[s % chunks, j], near(j, inner)) for j in range(1, half)]

    def other_copies(s):
        return [
            block_copy(s, me_c, send_own.at[s % chunks, 0], partner),
            block_copy(s, me_c, send_own.at[s % chunks, half], far_gate),
        ]

    def own_copies(s):
        return near_copies(s) + other_copies(s)

    def send_all(s):
        for copy in own_copies(s):
            copy.start()

    def drain_own(s):
        for copy in own_copies(s):
            copy.wait_send()

    def over(s, source):
        return block_copy(s, source, send_relay.at[s % chunks, source // INNER], partner)

    def along(s, source, j):
        return block_copy(s, source, send_along.at[s % chunks, source // INNER, j - 1], near(j, inner))

    def across(s, source):
        return block_copy(s, source, send_along.at[s % chunks, source // INNER, 0], far_gate)

    def pass_on(s, go, source, copies):
        if go:
            await_block(s, source)
        for copy in copies:
            if go:
                copy.start()
            else:
                copy.wait_send()

    mate = near(1, inner)
    far_corner = far(1 - side, inner) if half == 2 else far_gate
    even_of = lambda s: s % 2 == 0
    odd_of = lambda s: s % 2 == 1

    def full_first(s, go):
        @pl.when(is_gate)
        def _():
            for k in range(half):
                source = far(k, inner)
                pass_on(s, go, source, [along(s, source, j) for j in range(1, half)] + [over(s, source)])

        @pl.when(even_of(s))
        def _():
            for j in range(1, half):
                pass_on(s, go, near(j, inner), [over(s, near(j, inner))])

        @pl.when(odd_of(s))
        def _():
            pass_on(s, go, partner, [along(s, partner, j) for j in range(1, half)])

    def full_second(s, go):
        @pl.when(jnp.logical_not(is_gate))
        def _():
            for k in range(half):
                pass_on(s, go, far(k, inner), [over(s, far(k, inner))])

    def helped_first(s, go):
        @pl.when(jnp.logical_not(is_gate))
        def _():
            pass_on(s, go, partner, [along(s, partner, 1)])
            pass_on(s, go, mate, [over(s, mate)])

        @pl.when(is_gate & odd_of(s))
        def _():
            pass_on(s, go, partner, [across(s, partner)])

    def helped_second(s, go):
        @pl.when(is_gate & even_of(s))
        def _():
            pass_on(s, go, far_gate, [over(s, far_gate)])

        @pl.when(is_gate)
        def _():
            pass_on(s, go, far_corner, [over(s, far_corner)])

    def either(s, full, helped_one, go):
        if not assisted:
            full(s, go)
            return

        @pl.when(s < bound)
        def _():
            full(s, go)

        @pl.when(s >= bound)
        def _():
            helped_one(s, go)

    def first_relay(s, go):
        either(s, full_first, helped_first, go)

    def second_relay(s, go):
        either(s, full_second, helped_second, go)

    def await_rest(s):
        @pl.when(even_of(s))
        def _():
            await_block(s, partner)

        @pl.when(odd_of(s))
        def _():
            for j in range(1, half):
                await_block(s, near(j, inner))

        for j in range(1, half):
            await_block(s, near(j, other))
        for k in range(half):
            await_block(s, far(k, other))

    def await_helped(s):
        @pl.when(is_gate & even_of(s))
        def _():
            await_block(s, partner)

        @pl.when(is_gate & odd_of(s))
        def _():
            await_block(s, far_gate)

        await_block(s, near(1, other))

        @pl.when(is_gate)
        def _():
            await_block(s, mate)
            for k in range(half):
                await_block(s, far(k, other))

    far_base = (1 - side) * (width // 2)
    near_base = side * (width // 2)
    share = width // 2 // n_row
    bite = share // chunks
    sibling = me_r + 1 - 2 * (me_r % 2)
    cross = (me_r + 2) % n_row

    def helped_part(i, q):
        return helped.at[i // chunks, q, pl.ds((i % chunks) * bite, bite), :]

    def ship_copy(i):
        lines = pl.ds(pl.multiple_of(far_base + me_r * share + (i % chunks) * bite, bite), bite)
        source = weight.at[first_helped + i // chunks, lines, :]
        return remote(source, helped_part(i, me_r), send_help.at[i, 0], recv_help.at[i, me_r], me_r, mate)

    def help_copy(i, q, way, peer):
        block = helped_part(i, q)
        return remote(block, block, send_help.at[i, way], recv_help.at[i, q], peer, me_c)

    def spread_copies(i):
        return [help_copy(i, me_r, 1, sibling), help_copy(i, me_r, 2, cross)]

    def part_copy(s):
        slot = s - bound
        return remote(
            part_out.at[s % chunks], part_in.at[slot], send_part.at[s % chunks], recv_part.at[slot], me_r, mate
        )

    def scale_copy(s):
        slot = s - bound
        return remote(
            scale_out.at[s % chunks], scale_in.at[slot], send_scale.at[s % chunks], recv_scale.at[slot], me_r, mate
        )

    def at_steps(s, table, action):
        for when, items in table.items():
            @pl.when(s == when)
            def _():
                for i in items:
                    action(i)

    def spread(i):
        help_copy(i, me_r, 1, sibling).wait_recv()
        for copy in spread_copies(i):
            copy.start()

    def pass_cross(i):
        help_copy(i, cross, 3, sibling).wait_recv()
        help_copy(i, cross, 3, sibling).start()

    def move_weights(s):
        @pl.when(is_gate)
        def _():
            at_steps(s, RELAY, pass_cross)
            at_steps(s, SPREAD, spread)

        @pl.when(jnp.logical_not(is_gate))
        def _():
            at_steps(s, SHIP, lambda i: ship_copy(i).start())

    def await_weights(l):
        for i in range(assisted * chunks):
            @pl.when(is_gate & (l == first_helped + i // chunks))
            def _():
                for q in (sibling, (cross + 1 - 2 * (me_r % 2))):
                    help_copy(i, q, 1, sibling).wait_recv()

    def drain_weights():
        for i in range(assisted * chunks):
            @pl.when(is_gate)
            def _():
                for copy in spread_copies(i) + [help_copy(i, cross, 3, sibling)]:
                    copy.wait_send()

            @pl.when(jnp.logical_not(is_gate))
            def _():
                ship_copy(i).wait_send()

    def relay(s, relay_of):
        @pl.when(s < steps)
        def _():
            @pl.when(s >= chunks)
            def _():
                relay_of(s - chunks, False)

            relay_of(s, True)

    for j in range(1, n_row):
        id_row_copy(j).start()
    for ch in range(chunks):
        send_all(ch)

    for s in range(LEAD1):
        first_relay(jnp.int32(s), True)
    for s in range(LEAD2):
        second_relay(jnp.int32(s), True)

    def pass_ids():
        ids_here = id_own[...]
        for j in range(1, n_row):
            id_row_from(j).wait_recv()
            ids_here = ids_here + id_row[row_peer(j)]
        id_sum[...] = ids_here
        id_col[me_c] = ids_here
        for j in range(1, n_col):
            id_col_copy(j).start()

    def find_places():
        for j in range(1, n_col):
            id_col_from(j).wait_recv()
        tiles = []
        for tile in range(n_col // per_tile):
            joined = id_col[tile * per_tile]
            for c in range(tile * per_tile + 1, (tile + 1) * per_tile):
                joined = joined + id_col[c]
            tiles.append(joined)
        ids = jnp.concatenate(tiles, 1)

        bits = SUB.bit_length() - 1
        wide = (n_col * SUB).bit_length() - 1

        def origin(lane):
            group = lane >> wide
            source = (lane >> bits) & (n_col - 1)
            return source * rows_dev + group * SUB + (lane & (SUB - 1))

        low = lax.broadcasted_iota(jnp.int32, (slots, slots), 0)
        high = lax.broadcasted_iota(jnp.int32, (slots, slots), 1)
        shuffle = jnp.where(low == origin(high), 1.0, 0.0).astype(BF16)
        earlier = jnp.where(origin(low) < origin(high), 1.0, 0.0).astype(BF16)
        ids = jnp.dot(ids.astype(F32).astype(BF16), shuffle, preferred_element_type=F32).astype(jnp.int32)
        line = lax.broadcasted_iota(jnp.int32, (lead_dim, slots), 0)
        line_col = lax.broadcasted_iota(jnp.int32, (lead_dim, 1), 0)
        ids = jnp.where(line < n_row, ids, tasks)
        live = ids < tasks
        member = [jnp.where(ids == t, 1.0, 0.0) for t in range(tasks)]
        ranks = jnp.dot(jnp.concatenate(member, 0).astype(BF16), earlier, preferred_element_type=F32)
        base = jnp.zeros((1, 1), F32)
        position = jnp.zeros((lead_dim, slots), F32)
        for t in range(tasks):
            count = jnp.sum(member[t], axis=1, keepdims=True)
            offset = jnp.zeros((lead_dim, 1), F32) + base
            for r in range(n_row):
                here = count[r : r + 1, :]
                offset = offset + jnp.where(line_col > r, here, 0.0)
                base = base + here
            rank = ranks[t * lead_dim : (t + 1) * lead_dim, :]
            position = position + member[t] * (offset + rank)
        slot = jnp.floor((position + 0.5) * (1.0 / n_row))
        target = jnp.where(live, position - slot * n_row, -1.0).astype(jnp.int32)
        slot = jnp.where(target == me_r, slot.astype(jnp.int32), -1)
        slot_range = lax.broadcasted_iota(jnp.int32, (slots, n_row * m), 0)
        for ch in range(chunks):
            aimed = jnp.concatenate([slot[r : r + 1, ch * m : (ch + 1) * m] for r in range(n_row)], 1)
            put[ch] = jnp.where(slot_range == aimed, 1.0, 0.0).astype(BF16)

    def silu(values):
        half = 0.5 * values
        return (half + half * jnp.tanh(half)).astype(BF16)

    def opening(g, carry):
        if assisted:
            @pl.when(g == 0)
            def _():
                for l in range(first_helped, layers):
                    weight_copy(l).wait()

            @pl.when(jnp.logical_not(is_gate))
            def _():
                at_steps(g, {g: SHIP[g] for g in SHIP if g < groups}, lambda i: ship_copy(i).start())

        @pl.when(g == 0)
        def _():
            for s in range(LEAD1, chunks):
                first_relay(jnp.int32(s), True)
            weight_copy(0).wait()
            for l in range(layers):
                gain_copy(l).wait()

        for h in range(halves):
            if h > 0:
                second_relay(g * halves + h, True)
            else:
                @pl.when(g > 0)
                def _():
                    second_relay(g * halves, True)
        for h in range(halves):
            await_rest(g * halves + h)

        @pl.when(g == groups - 1)
        def _():
            relay(jnp.int32(chunks), first_relay)

            @pl.when(is_gate)
            def _():
                relay(jnp.int32(chunks + 1), first_relay)

        for c in range(n_col):
            lines = slice(c * SUB, (c + 1) * SUB)

            def piece(p):
                return hidden[g * halves + p // span, c, (p % span) * SUB : (p % span + 1) * SUB, :].astype(F32)

            total = jnp.zeros((SUB, part), F32)
            for p in range(n_col):
                values = piece(p)
                total = total + values * values
            inverse = lax.rsqrt(jnp.sum(total, axis=1, keepdims=True) * (1.0 / width) + epsilon)
            for p in range(n_col):
                cols = slice(p * part, (p + 1) * part)
                active[lines, cols] = silu(piece(p) * inverse * gain[0, :, cols])
        update = jnp.dot(active[...], weight[0], preferred_element_type=F32)
        own_lines = pl.ds(pl.multiple_of((me_c % span) * SUB, SUB), SUB)
        for h in range(halves):
            drain_own(g * halves + h)
        for c in range(n_col):
            own = hidden[g * halves + me_c // span, c, own_lines, :].astype(F32)
            result = (own + update[c * SUB : (c + 1) * SUB, :]).astype(BF16)
            hidden[chunks + g * halves + c // span, me_c, (c % span) * SUB : (c % span + 1) * SUB, :] = result
        for h in range(halves):
            send_all(chunks + g * halves + h)
        if assisted:
            @pl.when(is_gate)
            def _():
                at_steps(g, {g: SPREAD[g] for g in SPREAD if g < groups}, spread)

        return carry

    lax.fori_loop(0, groups, opening, 0)
    @pl.when(jnp.logical_not(is_gate))
    def _():
        relay(jnp.int32(chunks + 1), first_relay)

    for s in range(LEAD2):
        relay(jnp.int32(chunks + s), second_relay)

    def place(ch):
        for j in range(1, n_row):
            row_from(ch, j).wait_recv()
        arrived = income[ch].reshape(n_row * m, part)
        placed = jnp.dot(put[ch], arrived, preferred_element_type=F32)
        out_ref[...] = (out_ref[...].astype(F32) + placed).astype(BF16)

    def finish(s, l, ch, result):
        drain_own(s)

        @pl.when(l < layers - 1)
        def _():
            hidden[s + chunks, me_c] = result
            send_all(s + chunks)

        @pl.when(l == layers - 1)
        def _():
            income[ch, me_r] = result
            for j in range(1, n_row):
                row_copy(ch, j).start()

    def after(s, l, ch):
        @pl.when((l == layers - 1) & (ch >= 2))
        def _():
            place(ch - 2)

        @pl.when(s == chunks)
        def _():
            pass_ids()

        @pl.when(s == 2 * chunks)
        def _():
            find_places()

    def step(s, carry):
        l = s // chunks
        ch = s % chunks
        relay(s + LEAD2, second_relay)
        relay(s + LEAD1, first_relay)

        @pl.when((ch == 0) & (l < first_helped) if assisted else ch == 0)
        def _():
            weight_copy(l).wait()

        await_rest(s)
        total = jnp.zeros((m, part), F32)
        for c in range(n_col):
            values = hidden[s, c].astype(F32)
            total = total + values * values
        mean = jnp.sum(total, axis=1, keepdims=True) * (1.0 / width)
        inverse = lax.rsqrt(mean + epsilon)
        for c in range(n_col):
            cols = slice(c * part, (c + 1) * part)
            active[:m, cols] = silu(hidden[s, c].astype(F32) * inverse * gain[l, :, cols])
        update = jnp.dot(active[:m, :], weight[l], preferred_element_type=F32)
        result = (hidden[s, me_c].astype(F32) + update).astype(BF16)
        finish(s, l, ch, result)
        if assisted:
            move_weights(s)
        after(s, l, ch)
        return carry

    near_cols = pl.ds(pl.multiple_of(near_base, width // 2), width // 2)
    far_cols = pl.ds(pl.multiple_of(far_base, width // 2), width // 2)

    def activate(s, l, begin, inverse):
        for q in range(n_col // 2):
            c = begin * (n_col // 2) + q
            cols = columns(c)
            active[:m, cols] = silu(hidden[s, c].astype(F32) * inverse * gain[l, :, cols])

    def helped_step(s, carry):
        l = s // chunks
        ch = s % chunks
        square = lax.broadcasted_iota(jnp.int32, (m, m), 0) == lax.broadcasted_iota(jnp.int32, (m, m), 1)
        relay(s + LEAD2, second_relay)
        relay(s + LEAD1, first_relay)

        @pl.when(ch == 0)
        def _():
            await_weights(l)

        await_helped(s)

        @pl.when(is_gate)
        def _():
            total = jnp.zeros((m, part), F32)
            for c in range(n_col):
                values = hidden[s, c].astype(F32)
                total = total + values * values
            mean = jnp.sum(total, axis=1, keepdims=True) * (1.0 / width)
            inverse = lax.rsqrt(mean + epsilon)

            @pl.when(s >= bound + chunks)
            def _():
                scale_copy(s - chunks).wait_send()
                part_copy(s - chunks).wait_send()

            scale_out[ch, 0:1, 0:m] = jnp.sum(jnp.where(square, inverse, 0.0), axis=0, keepdims=True)
            scale_copy(s).start()
            activate(s, l, 1 - side, inverse)
            theirs = helped[l - first_helped].reshape(width // 2, part)
            part_out[ch] = jnp.dot(active[:m, far_cols], theirs, preferred_element_type=F32).astype(BF16)
            part_copy(s).start()
            activate(s, l, side, inverse)
            update = jnp.dot(active[:m, :], weight[l], preferred_element_type=F32)
            finish(s, l, ch, (hidden[s, me_c].astype(F32) + update).astype(BF16))

        @pl.when(jnp.logical_not(is_gate))
        def _():
            scale_copy(s).wait_recv()
            inverse = jnp.sum(jnp.where(square, scale_in[s - bound, 0:1, 0:m], 0.0), axis=1, keepdims=True)
            activate(s, l, side, inverse)
            update = jnp.dot(active[:m, near_cols], weight[l, near_cols, :], preferred_element_type=F32)
            part_copy(s).wait_recv()
            update = update + part_in[s - bound].astype(F32)
            finish(s, l, ch, (hidden[s, me_c].astype(F32) + update).astype(BF16))

        @pl.when(s == steps - 2)
        def _():
            drain_weights()

        after(s, l, ch)
        return carry

    lax.fori_loop(chunks, bound, step, 0)
    if assisted:
        lax.fori_loop(bound, steps, helped_step, 0)
    for ch in range(chunks):
        first_relay(jnp.int32(steps - chunks + ch), False)
        second_relay(jnp.int32(steps - chunks + ch), False)
    for j in range(1, n_row):
        id_row_copy(j).wait_send()
    for j in range(1, n_col):
        id_col_copy(j).wait_send()
    if assisted:
        @pl.when(is_gate)
        def _():
            for ch in range(chunks):
                scale_copy(steps - chunks + ch).wait_send()
                part_copy(steps - chunks + ch).wait_send()

    for ch in range(chunks - 1):
        for j in range(1, n_row):
            row_copy(ch, j).wait_send()
    place(chunks - 2)
    place(chunks - 1)
    for j in range(1, n_row):
        row_copy(chunks - 1, j).wait_send()


def shards(rows, task_ids, task_embed, norm_gain, layer_weight):
    rows_dev, width = rows.shape
    tasks = task_embed.shape[0]
    layers = layer_weight.shape[0]
    part = layer_weight.shape[2]
    n_row = lax.axis_size("row")
    n_col = lax.axis_size("col")
    slots = rows_dev * n_col
    chunks = CHUNKS
    m = slots // chunks
    lead_dim = -(-n_row // 8) * 8
    lanes = 128
    assisted = 1 if n_col // INNER == 4 and n_row == 4 and chunks == 4 and layers >= 4 and m <= 128 else 0
    sizes = (n_row, n_col, layers, chunks, tasks, assisted)
    spots = max(assisted * chunks, 1)
    buffers = [
        pltpu.VMEM((rows_dev, width), BF16),
        pltpu.VMEM((1, rows_dev), jnp.int32),
        pltpu.VMEM((tasks, width), BF16),
        pltpu.VMEM((layers, 1, width), F32),
        pltpu.VMEM((layers, width, part), BF16),
        pltpu.VMEM((layers * chunks, n_col, m, part), BF16),
        pltpu.VMEM((n_col * SUB, width), BF16),
        pltpu.VMEM((chunks, n_row, m, part), BF16),
        pltpu.VMEM((chunks, slots, n_row * m), BF16),
        pltpu.VMEM((max(assisted, 1), n_row, width // 2 // n_row if assisted else 16, part), BF16),
        pltpu.VMEM((chunks, m, part), BF16),
        pltpu.VMEM((spots, m, part), BF16),
        pltpu.VMEM((chunks, 8, lanes), F32),
        pltpu.VMEM((spots, 8, lanes), F32),
        pltpu.VMEM((lead_dim, lanes), jnp.int32),
        pltpu.VMEM((n_row, lead_dim, lanes), jnp.int32),
        pltpu.VMEM((lead_dim, lanes), jnp.int32),
        pltpu.VMEM((n_col, lead_dim, lanes), jnp.int32),
    ]
    held = sum(math.prod(b.shape) * jnp.dtype(b.dtype).itemsize for b in buffers)
    dma = pltpu.SemaphoreType.DMA
    vmem = pl.BlockSpec(memory_space=pltpu.VMEM)
    hbm = pl.BlockSpec(memory_space=pltpu.HBM)
    operands = [rows, task_ids.reshape(1, rows_dev), task_embed, norm_gain, layer_weight]
    return pl.pallas_call(
        functools.partial(kernel, sizes),
        out_shape=jax.ShapeDtypeStruct((slots, part), BF16),
        in_specs=[hbm] * 5,
        out_specs=vmem,
        scratch_shapes=buffers
        + [
            dma((3,)),
            dma((layers,)),
            dma((layers,)),
            dma((n_row,)),
            dma((n_row,)),
            dma((n_col,)),
            dma((n_col,)),
            dma((chunks, n_row)),
            dma((chunks, n_row)),
            dma((chunks, n_col // INNER // 2 + 1)),
            dma((chunks, n_col // INNER)),
            dma((chunks, n_col // INNER, max(1, n_col // INNER // 2 - 1))),
            dma((2 * chunks, n_col)),
            dma((spots, 4)),
            dma((spots, n_row)),
            dma((chunks,)),
            dma((spots,)),
            dma((chunks,)),
            dma((spots,)),
        ],
        compiler_params=pltpu.CompilerParams(
            collective_id=0, has_side_effects=True, vmem_limit_bytes=min(held + SPARE, 60 * 2**20)
        ),
    )(*[pltpu.with_memory_space_constraint(operand, pltpu.HBM) for operand in operands])


def solution(mesh):
    return jax.shard_map(
        shards,
        mesh=mesh,
        in_specs=(P(("row", "col"), None), P(("row", "col")), P(), P(), P(None, None, "col")),
        out_specs=P("row", "col"),
        check_vma=False,
    )
```

```python
import functools
import math

import jax
import jax.numpy as jnp
from jax import lax
from jax.experimental import pallas as pl
from jax.experimental.pallas import tpu as pltpu
from jax.sharding import PartitionSpec as P

epsilon = 1e-06
MESH = pl.DeviceIdType.MESH
INNER = 2
CHUNKS = 4
SUB = 16
SPARE = 10 * 2**20
LEAD1 = 2
LEAD2 = 1
SHIP = {0: (0,), 1: (1, 2), 5: (3,)}
SPREAD = {1: (0,), 4: (1,), 6: (2,), 9: (3,)}
RELAY = {5: (0,), 6: (1,), 8: (2,), 11: (3,)}
F32 = jnp.float32
BF16 = jnp.bfloat16


def kernel(
    sizes,
    rows_hbm,
    ids_hbm,
    embed_hbm,
    gain_hbm,
    weight_ref,
    out_ref,
    rows_ref,
    ids_ref,
    embed_ref,
    gain,
    weight,
    hidden,
    active,
    income,
    put,
    helped,
    part_out,
    part_in,
    scale_out,
    scale_in,
    id_own,
    id_row,
    id_sum,
    id_col,
    sem_input,
    sem_gain,
    sem_weight,
    send_idrow,
    recv_idrow,
    send_idcol,
    recv_idcol,
    send_row,
    recv_row,
    send_own,
    send_relay,
    send_along,
    recv_hidden,
    send_help,
    recv_help,
    send_part,
    recv_part,
    send_scale,
    recv_scale,
):
    n_row, n_col, layers, chunks, tasks, assisted = sizes
    n_outer = n_col // INNER
    rows_dev = rows_ref.shape[0]
    width = rows_ref.shape[1]
    part = width // n_col
    slots = rows_dev * n_col
    m = slots // chunks
    steps = layers * chunks
    first_helped = layers - assisted
    bound = first_helped * chunks
    groups = rows_dev // SUB
    halves = chunks // groups
    span = n_col // halves
    me_r = lax.axis_index("row")
    me_c = lax.axis_index("col")
    outer = me_c // INNER
    inner = me_c % INNER
    partner = outer * INNER + (INNER - 1 - inner)

    def columns(c):
        return pl.ds(pl.multiple_of(c * part, part), part)

    def col_peer(j):
        return (me_c + j) % n_col

    def row_peer(j):
        return (me_r + j) % n_row

    def remote(src, dst, send, recv, r, c):
        return pltpu.make_async_remote_copy(
            src_ref=src, dst_ref=dst, send_sem=send, recv_sem=recv, device_id=(r, c), device_id_type=MESH
        )

    def weight_copy(l):
        return pltpu.make_async_copy(weight_ref.at[l], weight.at[l], sem_weight.at[l])

    barrier = pltpu.get_barrier_semaphore()
    for j in range(1, n_row):
        pl.semaphore_signal(barrier, inc=1, device_id=(row_peer(j), me_c), device_id_type=MESH)
    for j in range(1, n_col):
        pl.semaphore_signal(barrier, inc=1, device_id=(me_r, col_peer(j)), device_id_type=MESH)

    inputs = [
        pltpu.make_async_copy(source, dest, sem_input.at[i])
        for i, (source, dest) in enumerate(((rows_hbm, rows_ref), (embed_hbm, embed_ref), (ids_hbm, ids_ref)))
    ]
    for copy in inputs:
        copy.start()

    def gain_copy(l):
        return pltpu.make_async_copy(gain_hbm.at[pl.ds(l, 1)], gain.at[l], sem_gain.at[l])

    out_ref[...] = jnp.zeros(out_ref.shape, BF16)
    for copy in inputs:
        copy.wait()
    for l in range(layers):
        gain_copy(l).start()
        weight_copy(l).start()

    lead_dim = id_own.shape[0]
    lanes = id_own.shape[1]
    per_tile = lanes // rows_dev
    raw_ids = ids_ref[...]
    spread = lax.broadcasted_iota(jnp.int32, (rows_dev, lanes), 1) - lax.broadcasted_iota(
        jnp.int32, (rows_dev, lanes), 0
    )
    spread = jnp.where(spread == (me_c % per_tile) * rows_dev, 1.0, 0.0).astype(BF16)
    own_ids = jnp.broadcast_to(raw_ids.astype(F32), (lead_dim, rows_dev)).astype(BF16)
    row_ids = jnp.dot(own_ids, spread, preferred_element_type=F32).astype(jnp.int32)
    sub = lax.broadcasted_iota(jnp.int32, (lead_dim, lanes), 0)
    id_own[...] = jnp.where(sub == me_r, row_ids, 0)

    eye = jnp.where(
        lax.broadcasted_iota(jnp.int32, (rows_dev, rows_dev), 0)
        == lax.broadcasted_iota(jnp.int32, (rows_dev, rows_dev), 1),
        1.0,
        0.0,
    ).astype(BF16)
    tall_ids = lax.dot_general(eye, own_ids, (((1,), (1,)), ((), ())), preferred_element_type=F32)[:, 0:1]
    embed_on = [jnp.where(tall_ids == float(t), 1.0, 0.0) for t in range(tasks)]
    for g in range(groups):
        lines = slice(g * SUB, (g + 1) * SUB)
        for c in range(n_col):
            cols = slice(c * part, (c + 1) * part)
            term = jnp.zeros((SUB, part), F32)
            for t in range(tasks):
                term = term + embed_on[t][lines, :] * embed_ref[t : t + 1, cols].astype(F32)
            begin = (rows_ref[lines, cols].astype(F32) + term).astype(BF16)
            hidden[g * halves + c // span, me_c, (c % span) * SUB : (c % span + 1) * SUB, :] = begin

    pl.semaphore_wait(barrier, n_row + n_col - 2)

    def id_row_copy(j):
        return remote(id_own, id_row.at[me_r], send_idrow.at[j], recv_idrow.at[me_r], row_peer(j), me_c)

    def id_row_from(j):
        return remote(id_own, id_row.at[row_peer(j)], send_idrow.at[j], recv_idrow.at[row_peer(j)], row_peer(j), me_c)

    def id_col_copy(j):
        return remote(id_sum, id_col.at[me_c], send_idcol.at[j], recv_idcol.at[me_c], me_r, col_peer(j))

    def id_col_from(j):
        return remote(id_sum, id_col.at[col_peer(j)], send_idcol.at[j], recv_idcol.at[col_peer(j)], me_r, col_peer(j))

    def row_copy(ch, j):
        block = income.at[ch, me_r]
        return remote(block, block, send_row.at[ch, j], recv_row.at[ch, me_r], row_peer(j), me_c)

    def row_from(ch, j):
        block = income.at[ch, row_peer(j)]
        return remote(block, block, send_row.at[ch, j], recv_row.at[ch, row_peer(j)], row_peer(j), me_c)

    half = n_outer // 2
    side = outer // half
    is_gate = outer == half - 1 + side
    far_gate = (half - side) * INNER + inner

    def near(j, i):
        return (side * half + (outer % half + j) % half) * INNER + i

    def far(k, i):
        return ((1 - side) * half + k) * INNER + i

    other = INNER - 1 - inner

    def block_copy(s, source, send, peer):
        block = hidden.at[s, source]
        return remote(block, block, send, recv_hidden.at[s % (2 * chunks), source], me_r, peer)

    def await_block(s, source):
        block_copy(s, source, send_relay.at[0, 0], partner).wait_recv()

    def near_copies(s):
        return [block_copy(s, me_c, send_own.at[s % chunks, j], near(j, inner)) for j in range(1, half)]

    def other_copies(s):
        return [
            block_copy(s, me_c, send_own.at[s % chunks, 0], partner),
            block_copy(s, me_c, send_own.at[s % chunks, half], far_gate),
        ]

    def own_copies(s):
        return near_copies(s) + other_copies(s)

    def send_all(s):
        for copy in own_copies(s):
            copy.start()

    def drain_own(s):
        for copy in own_copies(s):
            copy.wait_send()

    def over(s, source):
        return block_copy(s, source, send_relay.at[s % chunks, source // INNER], partner)

    def along(s, source, j):
        return block_copy(s, source, send_along.at[s % chunks, source // INNER, j - 1], near(j, inner))

    def across(s, source):
        return block_copy(s, source, send_along.at[s % chunks, source // INNER, 0], far_gate)

    def pass_on(s, go, source, copies):
        if go:
            await_block(s, source)
        for copy in copies:
            if go:
                copy.start()
            else:
                copy.wait_send()

    mate = near(1, inner)
    far_corner = far(1 - side, inner) if half == 2 else far_gate
    even_of = lambda s: s % 2 == 0
    odd_of = lambda s: s % 2 == 1

    def full_first(s, go):
        @pl.when(is_gate)
        def _():
            for k in range(half):
                source = far(k, inner)
                pass_on(s, go, source, [along(s, source, j) for j in range(1, half)] + [over(s, source)])

        @pl.when(even_of(s))
        def _():
            for j in range(1, half):
                pass_on(s, go, near(j, inner), [over(s, near(j, inner))])

        @pl.when(odd_of(s))
        def _():
            pass_on(s, go, partner, [along(s, partner, j) for j in range(1, half)])

    def full_second(s, go):
        @pl.when(jnp.logical_not(is_gate))
        def _():
            for k in range(half):
                pass_on(s, go, far(k, inner), [over(s, far(k, inner))])

    def helped_first(s, go):
        @pl.when(jnp.logical_not(is_gate))
        def _():
            pass_on(s, go, partner, [along(s, partner, 1)])
            pass_on(s, go, mate, [over(s, mate)])

        @pl.when(is_gate & odd_of(s))
        def _():
            pass_on(s, go, partner, [across(s, partner)])

    def helped_second(s, go):
        @pl.when(is_gate & even_of(s))
        def _():
            pass_on(s, go, far_gate, [over(s, far_gate)])

        @pl.when(is_gate)
        def _():
            pass_on(s, go, far_corner, [over(s, far_corner)])

    def either(s, full, helped_one, go):
        if not assisted:
            full(s, go)
            return

        @pl.when(s < bound)
        def _():
            full(s, go)

        @pl.when(s >= bound)
        def _():
            helped_one(s, go)

    def first_relay(s, go):
        either(s, full_first, helped_first, go)

    def second_relay(s, go):
        either(s, full_second, helped_second, go)

    def await_rest(s):
        @pl.when(even_of(s))
        def _():
            await_block(s, partner)

        @pl.when(odd_of(s))
        def _():
            for j in range(1, half):
                await_block(s, near(j, inner))

        for j in range(1, half):
            await_block(s, near(j, other))
        for k in range(half):
            await_block(s, far(k, other))

    def await_helped(s):
        @pl.when(is_gate & even_of(s))
        def _():
            await_block(s, partner)

        @pl.when(is_gate & odd_of(s))
        def _():
            await_block(s, far_gate)

        await_block(s, near(1, other))

        @pl.when(is_gate)
        def _():
            await_block(s, mate)
            for k in range(half):
                await_block(s, far(k, other))

    far_base = (1 - side) * (width // 2)
    near_base = side * (width // 2)
    share = width // 2 // n_row
    bite = share // chunks
    sibling = me_r + 1 - 2 * (me_r % 2)
    cross = (me_r + 2) % n_row

    def helped_part(i, q):
        return helped.at[i // chunks, q, pl.ds((i % chunks) * bite, bite), :]

    def ship_copy(i):
        lines = pl.ds(pl.multiple_of(far_base + me_r * share + (i % chunks) * bite, bite), bite)
        source = weight.at[first_helped + i // chunks, lines, :]
        return remote(source, helped_part(i, me_r), send_help.at[i, 0], recv_help.at[i, me_r], me_r, mate)

    def help_copy(i, q, way, peer):
        block = helped_part(i, q)
        return remote(block, block, send_help.at[i, way], recv_help.at[i, q], peer, me_c)

    def spread_copies(i):
        return [help_copy(i, me_r, 1, sibling), help_copy(i, me_r, 2, cross)]

    def part_copy(s):
        slot = s - bound
        return remote(
            part_out.at[s % chunks], part_in.at[slot], send_part.at[s % chunks], recv_part.at[slot], me_r, mate
        )

    def scale_copy(s):
        slot = s - bound
        return remote(
            scale_out.at[s % chunks], scale_in.at[slot], send_scale.at[s % chunks], recv_scale.at[slot], me_r, mate
        )

    def at_steps(s, table, action):
        for when, items in table.items():
            @pl.when(s == when)
            def _():
                for i in items:
                    action(i)

    def spread(i):
        help_copy(i, me_r, 1, sibling).wait_recv()
        for copy in spread_copies(i):
            copy.start()

    def pass_cross(i):
        help_copy(i, cross, 3, sibling).wait_recv()
        help_copy(i, cross, 3, sibling).start()

    def move_weights(s):
        @pl.when(is_gate)
        def _():
            at_steps(s, RELAY, pass_cross)
            at_steps(s, SPREAD, spread)

        @pl.when(jnp.logical_not(is_gate))
        def _():
            at_steps(s, SHIP, lambda i: ship_copy(i).start())

    def await_weights(l):
        for i in range(assisted * chunks):
            @pl.when(is_gate & (l == first_helped + i // chunks))
            def _():
                for q in (sibling, (cross + 1 - 2 * (me_r % 2))):
                    help_copy(i, q, 1, sibling).wait_recv()

    def drain_weights():
        for i in range(assisted * chunks):
            @pl.when(is_gate)
            def _():
                for copy in spread_copies(i) + [help_copy(i, cross, 3, sibling)]:
                    copy.wait_send()

            @pl.when(jnp.logical_not(is_gate))
            def _():
                ship_copy(i).wait_send()

    def relay(s, relay_of):
        @pl.when(s < steps)
        def _():
            @pl.when(s >= chunks)
            def _():
                relay_of(s - chunks, False)

            relay_of(s, True)

    for j in range(1, n_row):
        id_row_copy(j).start()
    for ch in range(chunks):
        send_all(ch)

    for s in range(LEAD1):
        first_relay(jnp.int32(s), True)
    for s in range(LEAD2):
        second_relay(jnp.int32(s), True)

    def pass_ids():
        ids_here = id_own[...]
        for j in range(1, n_row):
            id_row_from(j).wait_recv()
            ids_here = ids_here + id_row[row_peer(j)]
        id_sum[...] = ids_here
        id_col[me_c] = ids_here
        for j in range(1, n_col):
            id_col_copy(j).start()

    def find_places():
        for j in range(1, n_col):
            id_col_from(j).wait_recv()
        tiles = []
        for tile in range(n_col // per_tile):
            joined = id_col[tile * per_tile]
            for c in range(tile * per_tile + 1, (tile + 1) * per_tile):
                joined = joined + id_col[c]
            tiles.append(joined)
        ids = jnp.concatenate(tiles, 1)

        bits = SUB.bit_length() - 1
        wide = (n_col * SUB).bit_length() - 1

        def origin(lane):
            group = lane >> wide
            source = (lane >> bits) & (n_col - 1)
            return source * rows_dev + group * SUB + (lane & (SUB - 1))

        low = lax.broadcasted_iota(jnp.int32, (slots, slots), 0)
        high = lax.broadcasted_iota(jnp.int32, (slots, slots), 1)
        shuffle = jnp.where(low == origin(high), 1.0, 0.0).astype(BF16)
        earlier = jnp.where(origin(low) < origin(high), 1.0, 0.0).astype(BF16)
        ids = jnp.dot(ids.astype(F32).astype(BF16), shuffle, preferred_element_type=F32).astype(jnp.int32)
        line = lax.broadcasted_iota(jnp.int32, (lead_dim, slots), 0)
        line_col = lax.broadcasted_iota(jnp.int32, (lead_dim, 1), 0)
        ids = jnp.where(line < n_row, ids, tasks)
        live = ids < tasks
        member = [jnp.where(ids == t, 1.0, 0.0) for t in range(tasks)]
        ranks = jnp.dot(jnp.concatenate(member, 0).astype(BF16), earlier, preferred_element_type=F32)
        base = jnp.zeros((1, 1), F32)
        position = jnp.zeros((lead_dim, slots), F32)
        for t in range(tasks):
            count = jnp.sum(member[t], axis=1, keepdims=True)
            offset = jnp.zeros((lead_dim, 1), F32) + base
            for r in range(n_row):
                here = count[r : r + 1, :]
                offset = offset + jnp.where(line_col > r, here, 0.0)
                base = base + here
            rank = ranks[t * lead_dim : (t + 1) * lead_dim, :]
            position = position + member[t] * (offset + rank)
        slot = jnp.floor((position + 0.5) * (1.0 / n_row))
        target = jnp.where(live, position - slot * n_row, -1.0).astype(jnp.int32)
        slot = jnp.where(target == me_r, slot.astype(jnp.int32), -1)
        slot_range = lax.broadcasted_iota(jnp.int32, (slots, n_row * m), 0)
        for ch in range(chunks):
            aimed = jnp.concatenate([slot[r : r + 1, ch * m : (ch + 1) * m] for r in range(n_row)], 1)
            put[ch] = jnp.where(slot_range == aimed, 1.0, 0.0).astype(BF16)

    def silu(values):
        half = 0.5 * values
        return (half + half * jnp.tanh(half)).astype(BF16)

    def opening(g, carry):
        if assisted:
            @pl.when(g == 0)
            def _():
                for l in range(first_helped, layers):
                    weight_copy(l).wait()

            @pl.when(jnp.logical_not(is_gate))
            def _():
                at_steps(g, {g: SHIP[g] for g in SHIP if g < groups}, lambda i: ship_copy(i).start())

        @pl.when(g == 0)
        def _():
            for s in range(LEAD1, chunks):
                first_relay(jnp.int32(s), True)
            weight_copy(0).wait()
            for l in range(layers):
                gain_copy(l).wait()

        for h in range(halves):
            if h > 0:
                second_relay(g * halves + h, True)
            else:
                @pl.when(g > 0)
                def _():
                    second_relay(g * halves, True)
        for h in range(halves):
            await_rest(g * halves + h)

        @pl.when(g == groups - 1)
        def _():
            relay(jnp.int32(chunks), first_relay)

            @pl.when(is_gate)
            def _():
                relay(jnp.int32(chunks + 1), first_relay)

        for c in range(n_col):
            lines = slice(c * SUB, (c + 1) * SUB)

            def piece(p):
                return hidden[g * halves + p // span, c, (p % span) * SUB : (p % span + 1) * SUB, :].astype(F32)

            total = jnp.zeros((SUB, part), F32)
            for p in range(n_col):
                values = piece(p)
                total = total + values * values
            inverse = lax.rsqrt(jnp.sum(total, axis=1, keepdims=True) * (1.0 / width) + epsilon)
            for p in range(n_col):
                cols = slice(p * part, (p + 1) * part)
                active[lines, cols] = silu(piece(p) * inverse * gain[0, :, cols])
        update = jnp.dot(active[...], weight[0], preferred_element_type=F32)
        own_lines = pl.ds(pl.multiple_of((me_c % span) * SUB, SUB), SUB)
        for h in range(halves):
            drain_own(g * halves + h)
        for c in range(n_col):
            own = hidden[g * halves + me_c // span, c, own_lines, :].astype(F32)
            result = (own + update[c * SUB : (c + 1) * SUB, :]).astype(BF16)
            hidden[chunks + g * halves + c // span, me_c, (c % span) * SUB : (c % span + 1) * SUB, :] = result
        for h in range(halves):
            send_all(chunks + g * halves + h)
        if assisted:
            @pl.when(is_gate)
            def _():
                at_steps(g, {g: SPREAD[g] for g in SPREAD if g < groups}, spread)

        return carry

    lax.fori_loop(0, groups, opening, 0)
    @pl.when(jnp.logical_not(is_gate))
    def _():
        relay(jnp.int32(chunks + 1), first_relay)

    for s in range(LEAD2):
        relay(jnp.int32(chunks + s), second_relay)

    def place(ch):
        for j in range(1, n_row):
            row_from(ch, j).wait_recv()
        arrived = income[ch].reshape(n_row * m, part)
        placed = jnp.dot(put[ch], arrived, preferred_element_type=F32)
        out_ref[...] = (out_ref[...].astype(F32) + placed).astype(BF16)

    def finish(s, l, ch, result):
        drain_own(s)

        @pl.when(l < layers - 1)
        def _():
            hidden[s + chunks, me_c] = result
            send_all(s + chunks)

        @pl.when(l == layers - 1)
        def _():
            income[ch, me_r] = result
            for j in range(1, n_row):
                row_copy(ch, j).start()

    def after(s, l, ch):
        @pl.when((l == layers - 1) & (ch >= 2))
        def _():
            place(ch - 2)

        @pl.when(s == chunks)
        def _():
            pass_ids()

        @pl.when(s == 2 * chunks)
        def _():
            find_places()

    def step(s, carry):
        l = s // chunks
        ch = s % chunks
        relay(s + LEAD2, second_relay)
        relay(s + LEAD1, first_relay)

        @pl.when((ch == 0) & (l < first_helped) if assisted else ch == 0)
        def _():
            weight_copy(l).wait()

        await_rest(s)
        total = jnp.zeros((m, part), F32)
        for c in range(n_col):
            values = hidden[s, c].astype(F32)
            total = total + values * values
        mean = jnp.sum(total, axis=1, keepdims=True) * (1.0 / width)
        inverse = lax.rsqrt(mean + epsilon)
        for c in range(n_col):
            cols = slice(c * part, (c + 1) * part)
            active[:m, cols] = silu(hidden[s, c].astype(F32) * inverse * gain[l, :, cols])
        update = jnp.dot(active[:m, :], weight[l], preferred_element_type=F32)
        result = (hidden[s, me_c].astype(F32) + update).astype(BF16)
        finish(s, l, ch, result)
        if assisted:
            move_weights(s)
        after(s, l, ch)
        return carry

    near_cols = pl.ds(pl.multiple_of(near_base, width // 2), width // 2)
    far_cols = pl.ds(pl.multiple_of(far_base, width // 2), width // 2)

    def activate(s, l, begin, inverse):
        for q in range(n_col // 2):
            c = begin * (n_col // 2) + q
            cols = columns(c)
            active[:m, cols] = silu(hidden[s, c].astype(F32) * inverse * gain[l, :, cols])

    def helped_step(s, carry):
        l = s // chunks
        ch = s % chunks
        square = lax.broadcasted_iota(jnp.int32, (m, m), 0) == lax.broadcasted_iota(jnp.int32, (m, m), 1)
        relay(s + LEAD2, second_relay)
        relay(s + LEAD1, first_relay)

        @pl.when(ch == 0)
        def _():
            await_weights(l)

        await_helped(s)

        @pl.when(is_gate)
        def _():
            total = jnp.zeros((m, part), F32)
            for c in range(n_col):
                values = hidden[s, c].astype(F32)
                total = total + values * values
            mean = jnp.sum(total, axis=1, keepdims=True) * (1.0 / width)
            inverse = lax.rsqrt(mean + epsilon)

            @pl.when(s >= bound + chunks)
            def _():
                scale_copy(s - chunks).wait_send()
                part_copy(s - chunks).wait_send()

            scale_out[ch, 0:1, 0:m] = jnp.sum(jnp.where(square, inverse, 0.0), axis=0, keepdims=True)
            scale_copy(s).start()
            activate(s, l, 1 - side, inverse)
            theirs = helped[l - first_helped].reshape(width // 2, part)
            part_out[ch] = jnp.dot(active[:m, far_cols], theirs, preferred_element_type=F32).astype(BF16)
            part_copy(s).start()
            activate(s, l, side, inverse)
            update = jnp.dot(active[:m, :], weight[l], preferred_element_type=F32)
            finish(s, l, ch, (hidden[s, me_c].astype(F32) + update).astype(BF16))

        @pl.when(jnp.logical_not(is_gate))
        def _():
            scale_copy(s).wait_recv()
            inverse = jnp.sum(jnp.where(square, scale_in[s - bound, 0:1, 0:m], 0.0), axis=1, keepdims=True)
            activate(s, l, side, inverse)
            update = jnp.dot(active[:m, near_cols], weight[l, near_cols, :], preferred_element_type=F32)
            part_copy(s).wait_recv()
            update = update + part_in[s - bound].astype(F32)
            finish(s, l, ch, (hidden[s, me_c].astype(F32) + update).astype(BF16))

        @pl.when(s == steps - 2)
        def _():
            drain_weights()

        after(s, l, ch)
        return carry

    lax.fori_loop(chunks, bound, step, 0)
    if assisted:
        lax.fori_loop(bound, steps, helped_step, 0)
    for ch in range(chunks):
        first_relay(jnp.int32(steps - chunks + ch), False)
        second_relay(jnp.int32(steps - chunks + ch), False)
    for j in range(1, n_row):
        id_row_copy(j).wait_send()
    for j in range(1, n_col):
        id_col_copy(j).wait_send()
    if assisted:
        @pl.when(is_gate)
        def _():
            for ch in range(chunks):
                scale_copy(steps - chunks + ch).wait_send()
                part_copy(steps - chunks + ch).wait_send()

    for ch in range(chunks - 1):
        for j in range(1, n_row):
            row_copy(ch, j).wait_send()
    place(chunks - 2)
    place(chunks - 1)
    for j in range(1, n_row):
        row_copy(chunks - 1, j).wait_send()


def shards(rows, task_ids, task_embed, norm_gain, layer_weight):
    rows_dev, width = rows.shape
    tasks = task_embed.shape[0]
    layers = layer_weight.shape[0]
    part = layer_weight.shape[2]
    n_row = lax.axis_size("row")
    n_col = lax.axis_size("col")
    slots = rows_dev * n_col
    chunks = CHUNKS
    m = slots // chunks
    lead_dim = -(-n_row // 8) * 8
    lanes = 128
    assisted = 1 if n_col // INNER == 4 and n_row == 4 and chunks == 4 and layers >= 4 and m <= 128 else 0
    sizes = (n_row, n_col, layers, chunks, tasks, assisted)
    spots = max(assisted * chunks, 1)
    buffers = [
        pltpu.VMEM((rows_dev, width), BF16),
        pltpu.VMEM((1, rows_dev), jnp.int32),
        pltpu.VMEM((tasks, width), BF16),
        pltpu.VMEM((layers, 1, width), F32),
        pltpu.VMEM((layers, width, part), BF16),
        pltpu.VMEM((layers * chunks, n_col, m, part), BF16),
        pltpu.VMEM((n_col * SUB, width), BF16),
        pltpu.VMEM((chunks, n_row, m, part), BF16),
        pltpu.VMEM((chunks, slots, n_row * m), BF16),
        pltpu.VMEM((max(assisted, 1), n_row, width // 2 // n_row if assisted else 16, part), BF16),
        pltpu.VMEM((chunks, m, part), BF16),
        pltpu.VMEM((spots, m, part), BF16),
        pltpu.VMEM((chunks, 8, lanes), F32),
        pltpu.VMEM((spots, 8, lanes), F32),
        pltpu.VMEM((lead_dim, lanes), jnp.int32),
        pltpu.VMEM((n_row, lead_dim, lanes), jnp.int32),
        pltpu.VMEM((lead_dim, lanes), jnp.int32),
        pltpu.VMEM((n_col, lead_dim, lanes), jnp.int32),
    ]
    held = sum(math.prod(b.shape) * jnp.dtype(b.dtype).itemsize for b in buffers)
    dma = pltpu.SemaphoreType.DMA
    vmem = pl.BlockSpec(memory_space=pltpu.VMEM)
    hbm = pl.BlockSpec(memory_space=pltpu.HBM)
    operands = [rows, task_ids.reshape(1, rows_dev), task_embed, norm_gain, layer_weight]
    return pl.pallas_call(
        functools.partial(kernel, sizes),
        out_shape=jax.ShapeDtypeStruct((slots, part), BF16),
        in_specs=[hbm] * 5,
        out_specs=vmem,
        scratch_shapes=buffers
        + [
            dma((3,)),
            dma((layers,)),
            dma((layers,)),
            dma((n_row,)),
            dma((n_row,)),
            dma((n_col,)),
            dma((n_col,)),
            dma((chunks, n_row)),
            dma((chunks, n_row)),
            dma((chunks, n_col // INNER // 2 + 1)),
            dma((chunks, n_col // INNER)),
            dma((chunks, n_col // INNER, max(1, n_col // INNER // 2 - 1))),
            dma((2 * chunks, n_col)),
            dma((spots, 4)),
            dma((spots, n_row)),
            dma((chunks,)),
            dma((spots,)),
            dma((chunks,)),
            dma((spots,)),
        ],
        compiler_params=pltpu.CompilerParams(
            collective_id=0, has_side_effects=True, vmem_limit_bytes=min(held + SPARE, 60 * 2**20)
        ),
    )(*[pltpu.with_memory_space_constraint(operand, pltpu.HBM) for operand in operands])


def solution(mesh):
    return jax.shard_map(
        shards,
        mesh=mesh,
        in_specs=(P(("row", "col"), None), P(("row", "col")), P(), P(), P(None, None, "col")),
        out_specs=P("row", "col"),
        check_vma=False,
    )
```

```python
import functools
import math

import jax
import jax.numpy as jnp
from jax import lax
from jax.experimental import pallas as pl
from jax.experimental.pallas import tpu as pltpu
from jax.sharding import PartitionSpec as P

epsilon = 1e-06
MESH = pl.DeviceIdType.MESH
INNER = 2
CHUNKS = 4
SUB = 16
SPARE = 10 * 2**20
LEAD1 = 2
LEAD2 = 1
SHIP = {0: (0,), 1: (1, 2), 5: (3,)}
SPREAD = {1: (0,), 4: (1,), 6: (2,), 9: (3,)}
RELAY = {5: (0,), 6: (1,), 8: (2,), 11: (3,)}
F32 = jnp.float32
BF16 = jnp.bfloat16


def kernel(
    sizes,
    rows_hbm,
    ids_hbm,
    embed_hbm,
    gain_hbm,
    weight_ref,
    out_ref,
    rows_ref,
    ids_ref,
    embed_ref,
    gain,
    weight,
    hidden,
    active,
    income,
    put,
    helped,
    part_out,
    part_in,
    scale_out,
    scale_in,
    id_own,
    id_row,
    id_sum,
    id_col,
    sem_input,
    sem_gain,
    sem_weight,
    send_idrow,
    recv_idrow,
    send_idcol,
    recv_idcol,
    send_row,
    recv_row,
    send_own,
    send_relay,
    send_along,
    recv_hidden,
    send_help,
    recv_help,
    send_part,
    recv_part,
    send_scale,
    recv_scale,
):
    n_row, n_col, layers, chunks, tasks, assisted = sizes
    n_outer = n_col // INNER
    rows_dev = rows_ref.shape[0]
    width = rows_ref.shape[1]
    part = width // n_col
    slots = rows_dev * n_col
    m = slots // chunks
    steps = layers * chunks
    first_helped = layers - assisted
    bound = first_helped * chunks
    groups = rows_dev // SUB
    halves = chunks // groups
    span = n_col // halves
    me_r = lax.axis_index("row")
    me_c = lax.axis_index("col")
    outer = me_c // INNER
    inner = me_c % INNER
    partner = outer * INNER + (INNER - 1 - inner)

    def columns(c):
        return pl.ds(pl.multiple_of(c * part, part), part)

    def col_peer(j):
        return (me_c + j) % n_col

    def row_peer(j):
        return (me_r + j) % n_row

    def remote(src, dst, send, recv, r, c):
        return pltpu.make_async_remote_copy(
            src_ref=src, dst_ref=dst, send_sem=send, recv_sem=recv, device_id=(r, c), device_id_type=MESH
        )

    def weight_copy(l):
        return pltpu.make_async_copy(weight_ref.at[l], weight.at[l], sem_weight.at[l])

    barrier = pltpu.get_barrier_semaphore()
    for j in range(1, n_row):
        pl.semaphore_signal(barrier, inc=1, device_id=(row_peer(j), me_c), device_id_type=MESH)
    for j in range(1, n_col):
        pl.semaphore_signal(barrier, inc=1, device_id=(me_r, col_peer(j)), device_id_type=MESH)

    inputs = [
        pltpu.make_async_copy(source, dest, sem_input.at[i])
        for i, (source, dest) in enumerate(((rows_hbm, rows_ref), (embed_hbm, embed_ref), (ids_hbm, ids_ref)))
    ]
    for copy in inputs:
        copy.start()

    def gain_copy(l):
        return pltpu.make_async_copy(gain_hbm.at[pl.ds(l, 1)], gain.at[l], sem_gain.at[l])

    out_ref[...] = jnp.zeros(out_ref.shape, BF16)
    for copy in inputs:
        copy.wait()
    for l in range(layers):
        gain_copy(l).start()
        weight_copy(l).start()

    lead_dim = id_own.shape[0]
    lanes = id_own.shape[1]
    per_tile = lanes // rows_dev
    raw_ids = ids_ref[...]
    spread = lax.broadcasted_iota(jnp.int32, (rows_dev, lanes), 1) - lax.broadcasted_iota(
        jnp.int32, (rows_dev, lanes), 0
    )
    spread = jnp.where(spread == (me_c % per_tile) * rows_dev, 1.0, 0.0).astype(BF16)
    own_ids = jnp.broadcast_to(raw_ids.astype(F32), (lead_dim, rows_dev)).astype(BF16)
    row_ids = jnp.dot(own_ids, spread, preferred_element_type=F32).astype(jnp.int32)
    sub = lax.broadcasted_iota(jnp.int32, (lead_dim, lanes), 0)
    id_own[...] = jnp.where(sub == me_r, row_ids, 0)

    eye = jnp.where(
        lax.broadcasted_iota(jnp.int32, (rows_dev, rows_dev), 0)
        == lax.broadcasted_iota(jnp.int32, (rows_dev, rows_dev), 1),
        1.0,
        0.0,
    ).astype(BF16)
    tall_ids = lax.dot_general(eye, own_ids, (((1,), (1,)), ((), ())), preferred_element_type=F32)[:, 0:1]
    embed_on = [jnp.where(tall_ids == float(t), 1.0, 0.0) for t in range(tasks)]
    for g in range(groups):
        lines = slice(g * SUB, (g + 1) * SUB)
        for c in range(n_col):
            cols = slice(c * part, (c + 1) * part)
            term = jnp.zeros((SUB, part), F32)
            for t in range(tasks):
                term = term + embed_on[t][lines, :] * embed_ref[t : t + 1, cols].astype(F32)
            begin = (rows_ref[lines, cols].astype(F32) + term).astype(BF16)
            hidden[g * halves + c // span, me_c, (c % span) * SUB : (c % span + 1) * SUB, :] = begin

    pl.semaphore_wait(barrier, n_row + n_col - 2)

    def id_row_copy(j):
        return remote(id_own, id_row.at[me_r], send_idrow.at[j], recv_idrow.at[me_r], row_peer(j), me_c)

    def id_row_from(j):
        return remote(id_own, id_row.at[row_peer(j)], send_idrow.at[j], recv_idrow.at[row_peer(j)], row_peer(j), me_c)

    def id_col_copy(j):
        return remote(id_sum, id_col.at[me_c], send_idcol.at[j], recv_idcol.at[me_c], me_r, col_peer(j))

    def id_col_from(j):
        return remote(id_sum, id_col.at[col_peer(j)], send_idcol.at[j], recv_idcol.at[col_peer(j)], me_r, col_peer(j))

    def row_copy(ch, j):
        block = income.at[ch, me_r]
        return remote(block, block, send_row.at[ch, j], recv_row.at[ch, me_r], row_peer(j), me_c)

    def row_from(ch, j):
        block = income.at[ch, row_peer(j)]
        return remote(block, block, send_row.at[ch, j], recv_row.at[ch, row_peer(j)], row_peer(j), me_c)

    half = n_outer // 2
    side = outer // half
    is_gate = outer == half - 1 + side
    far_gate = (half - side) * INNER + inner

    def near(j, i):
        return (side * half + (outer % half + j) % half) * INNER + i

    def far(k, i):
        return ((1 - side) * half + k) * INNER + i

    other = INNER - 1 - inner

    def block_copy(s, source, send, peer):
        block = hidden.at[s, source]
        return remote(block, block, send, recv_hidden.at[s % (2 * chunks), source], me_r, peer)

    def await_block(s, source):
        block_copy(s, source, send_relay.at[0, 0], partner).wait_recv()

    def near_copies(s):
        return [block_copy(s, me_c, send_own.at[s % chunks, j], near(j, inner)) for j in range(1, half)]

    def other_copies(s):
        return [
            block_copy(s, me_c, send_own.at[s % chunks, half], far_gate),
            block_copy(s, me_c, send_own.at[s % chunks, 0], partner),
        ]

    def own_copies(s):
        return other_copies(s) + near_copies(s)

    def send_all(s):
        for copy in own_copies(s):
            copy.start()

    def drain_own(s):
        for copy in own_copies(s):
            copy.wait_send()

    def over(s, source):
        return block_copy(s, source, send_relay.at[s % chunks, source // INNER], partner)

    def along(s, source, j):
        return block_copy(s, source, send_along.at[s % chunks, source // INNER, j - 1], near(j, inner))

    def across(s, source):
        return block_copy(s, source, send_along.at[s % chunks, source // INNER, 0], far_gate)

    def pass_on(s, go, source, copies):
        if go:
            await_block(s, source)
        for copy in copies:
            if go:
                copy.start()
            else:
                copy.wait_send()

    mate = near(1, inner)
    far_corner = far(1 - side, inner) if half == 2 else far_gate
    even_of = lambda s: s % 2 == 0
    odd_of = lambda s: s % 2 == 1

    def full_first(s, go):
        @pl.when(is_gate)
        def _():
            for k in range(half):
                source = far(k, inner)
                pass_on(s, go, source, [along(s, source, j) for j in range(1, half)] + [over(s, source)])

        @pl.when(even_of(s))
        def _():
            for j in range(1, half):
                pass_on(s, go, near(j, inner), [over(s, near(j, inner))])

        @pl.when(odd_of(s))
        def _():
            pass_on(s, go, partner, [along(s, partner, j) for j in range(1, half)])

    def full_second(s, go):
        @pl.when(jnp.logical_not(is_gate))
        def _():
            for k in range(half):
                pass_on(s, go, far(k, inner), [over(s, far(k, inner))])

    def helped_first(s, go):
        @pl.when(jnp.logical_not(is_gate))
        def _():
            pass_on(s, go, partner, [along(s, partner, 1)])
            pass_on(s, go, mate, [over(s, mate)])

        @pl.when(is_gate)
        def _():
            pass_on(s, go, partner, [across(s, partner)])

    def helped_second(s, go):
        @pl.when(is_gate)
        def _():
            pass_on(s, go, far_corner, [over(s, far_corner)])

    def either(s, full, helped_one, go):
        if not assisted:
            full(s, go)
            return

        @pl.when(s < bound)
        def _():
            full(s, go)

        @pl.when(s >= bound)
        def _():
            helped_one(s, go)

    def first_relay(s, go):
        either(s, full_first, helped_first, go)

    def second_relay(s, go):
        either(s, full_second, helped_second, go)

    def await_rest(s):
        @pl.when(even_of(s))
        def _():
            await_block(s, partner)

        @pl.when(odd_of(s))
        def _():
            for j in range(1, half):
                await_block(s, near(j, inner))

        for j in range(1, half):
            await_block(s, near(j, other))
        for k in range(half):
            await_block(s, far(k, other))

    def await_helped(s):
        await_block(s, near(1, other))

        @pl.when(is_gate)
        def _():
            await_block(s, far_gate)
            await_block(s, mate)
            for k in range(half):
                await_block(s, far(k, other))

    far_base = (1 - side) * (width // 2)
    near_base = side * (width // 2)
    share = width // 2 // n_row
    bite = share // chunks
    sibling = me_r + 1 - 2 * (me_r % 2)
    cross = (me_r + 2) % n_row

    def helped_part(i, q):
        return helped.at[i // chunks, q, pl.ds((i % chunks) * bite, bite), :]

    def ship_copy(i):
        lines = pl.ds(pl.multiple_of(far_base + me_r * share + (i % chunks) * bite, bite), bite)
        source = weight.at[first_helped + i // chunks, lines, :]
        return remote(source, helped_part(i, me_r), send_help.at[i, 0], recv_help.at[i, me_r], me_r, mate)

    def help_copy(i, q, way, peer):
        block = helped_part(i, q)
        return remote(block, block, send_help.at[i, way], recv_help.at[i, q], peer, me_c)

    def spread_copies(i):
        return [help_copy(i, me_r, 1, sibling), help_copy(i, me_r, 2, cross)]

    def part_copy(s):
        slot = s - bound
        return remote(
            part_out.at[s % chunks], part_in.at[slot], send_part.at[s % chunks], recv_part.at[slot], me_r, mate
        )

    def scale_copy(s):
        slot = s - bound
        return remote(
            scale_out.at[s % chunks], scale_in.at[slot], send_scale.at[s % chunks], recv_scale.at[slot], me_r, mate
        )

    def at_steps(s, table, action):
        for when, items in table.items():
            @pl.when(s == when)
            def _():
                for i in items:
                    action(i)

    def spread(i):
        help_copy(i, me_r, 1, sibling).wait_recv()
        for copy in spread_copies(i):
            copy.start()

    def pass_cross(i):
        help_copy(i, cross, 3, sibling).wait_recv()
        help_copy(i, cross, 3, sibling).start()

    def move_weights(s):
        @pl.when(is_gate)
        def _():
            at_steps(s, RELAY, pass_cross)
            at_steps(s, SPREAD, spread)

        @pl.when(jnp.logical_not(is_gate))
        def _():
            at_steps(s, SHIP, lambda i: ship_copy(i).start())

    def await_weights(l):
        for i in range(assisted * chunks):
            @pl.when(is_gate & (l == first_helped + i // chunks))
            def _():
                for q in (sibling, (cross + 1 - 2 * (me_r % 2))):
                    help_copy(i, q, 1, sibling).wait_recv()

    def drain_weights():
        for i in range(assisted * chunks):
            @pl.when(is_gate)
            def _():
                for copy in spread_copies(i) + [help_copy(i, cross, 3, sibling)]:
                    copy.wait_send()

            @pl.when(jnp.logical_not(is_gate))
            def _():
                ship_copy(i).wait_send()

    def relay(s, relay_of):
        @pl.when(s < steps)
        def _():
            @pl.when(s >= chunks)
            def _():
                relay_of(s - chunks, False)

            relay_of(s, True)

    for j in range(1, n_row):
        id_row_copy(j).start()
    def open_sends(ch):
        if ch < chunks - 1:
            send_all(ch)
        else:
            for copy in other_copies(ch):
                copy.start()

            @pl.when(jnp.logical_not(is_gate))
            def _():
                for copy in near_copies(ch):
                    copy.start()

    for ch in range(chunks):
        open_sends(ch)

    for s in range(LEAD1):
        first_relay(jnp.int32(s), True)
    for s in range(LEAD2):
        second_relay(jnp.int32(s), True)

    def pass_ids():
        ids_here = id_own[...]
        for j in range(1, n_row):
            id_row_from(j).wait_recv()
            ids_here = ids_here + id_row[row_peer(j)]
        id_sum[...] = ids_here
        id_col[me_c] = ids_here
        for j in range(1, n_col):
            id_col_copy(j).start()

    def find_places():
        for j in range(1, n_col):
            id_col_from(j).wait_recv()
        tiles = []
        for tile in range(n_col // per_tile):
            joined = id_col[tile * per_tile]
            for c in range(tile * per_tile + 1, (tile + 1) * per_tile):
                joined = joined + id_col[c]
            tiles.append(joined)
        ids = jnp.concatenate(tiles, 1)

        bits = SUB.bit_length() - 1
        wide = (n_col * SUB).bit_length() - 1

        def origin(lane):
            group = lane >> wide
            source = (lane >> bits) & (n_col - 1)
            return source * rows_dev + group * SUB + (lane & (SUB - 1))

        low = lax.broadcasted_iota(jnp.int32, (slots, slots), 0)
        high = lax.broadcasted_iota(jnp.int32, (slots, slots), 1)
        shuffle = jnp.where(low == origin(high), 1.0, 0.0).astype(BF16)
        earlier = jnp.where(origin(low) < origin(high), 1.0, 0.0).astype(BF16)
        ids = jnp.dot(ids.astype(F32).astype(BF16), shuffle, preferred_element_type=F32).astype(jnp.int32)
        line = lax.broadcasted_iota(jnp.int32, (lead_dim, slots), 0)
        line_col = lax.broadcasted_iota(jnp.int32, (lead_dim, 1), 0)
        ids = jnp.where(line < n_row, ids, tasks)
        live = ids < tasks
        member = [jnp.where(ids == t, 1.0, 0.0) for t in range(tasks)]
        ranks = jnp.dot(jnp.concatenate(member, 0).astype(BF16), earlier, preferred_element_type=F32)
        base = jnp.zeros((1, 1), F32)
        position = jnp.zeros((lead_dim, slots), F32)
        for t in range(tasks):
            count = jnp.sum(member[t], axis=1, keepdims=True)
            offset = jnp.zeros((lead_dim, 1), F32) + base
            for r in range(n_row):
                here = count[r : r + 1, :]
                offset = offset + jnp.where(line_col > r, here, 0.0)
                base = base + here
            rank = ranks[t * lead_dim : (t + 1) * lead_dim, :]
            position = position + member[t] * (offset + rank)
        slot = jnp.floor((position + 0.5) * (1.0 / n_row))
        target = jnp.where(live, position - slot * n_row, -1.0).astype(jnp.int32)
        slot = jnp.where(target == me_r, slot.astype(jnp.int32), -1)
        slot_range = lax.broadcasted_iota(jnp.int32, (slots, n_row * m), 0)
        for ch in range(chunks):
            aimed = jnp.concatenate([slot[r : r + 1, ch * m : (ch + 1) * m] for r in range(n_row)], 1)
            put[ch] = jnp.where(slot_range == aimed, 1.0, 0.0).astype(BF16)

    def silu(values):
        half = 0.5 * values
        return (half + half * jnp.tanh(half)).astype(BF16)

    def opening(g, carry):
        if assisted:
            @pl.when(g == 0)
            def _():
                for l in range(first_helped, layers):
                    weight_copy(l).wait()

            @pl.when(jnp.logical_not(is_gate))
            def _():
                at_steps(g, {g: SHIP[g] for g in SHIP if g < groups}, lambda i: ship_copy(i).start())

        @pl.when(g == 0)
        def _():
            for s in range(LEAD1, chunks):
                first_relay(jnp.int32(s), True)

            @pl.when(is_gate)
            def _():
                for copy in near_copies(chunks - 1):
                    copy.start()

            weight_copy(0).wait()
            for l in range(layers):
                gain_copy(l).wait()

        for h in range(halves):
            if h > 0:
                second_relay(g * halves + h, True)
            else:
                @pl.when(g > 0)
                def _():
                    second_relay(g * halves, True)
        for h in range(halves):
            await_rest(g * halves + h)

        @pl.when(g == groups - 1)
        def _():
            relay(jnp.int32(chunks), first_relay)

            @pl.when(is_gate)
            def _():
                relay(jnp.int32(chunks + 1), first_relay)

        for c in range(n_col):
            lines = slice(c * SUB, (c + 1) * SUB)

            def piece(p):
                return hidden[g * halves + p // span, c, (p % span) * SUB : (p % span + 1) * SUB, :].astype(F32)

            total = jnp.zeros((SUB, part), F32)
            for p in range(n_col):
                values = piece(p)
                total = total + values * values
            inverse = lax.rsqrt(jnp.sum(total, axis=1, keepdims=True) * (1.0 / width) + epsilon)
            for p in range(n_col):
                cols = slice(p * part, (p + 1) * part)
                active[lines, cols] = silu(piece(p) * inverse * gain[0, :, cols])
        update = jnp.dot(active[...], weight[0], preferred_element_type=F32)
        own_lines = pl.ds(pl.multiple_of((me_c % span) * SUB, SUB), SUB)
        for h in range(halves):
            drain_own(g * halves + h)
        for c in range(n_col):
            own = hidden[g * halves + me_c // span, c, own_lines, :].astype(F32)
            result = (own + update[c * SUB : (c + 1) * SUB, :]).astype(BF16)
            hidden[chunks + g * halves + c // span, me_c, (c % span) * SUB : (c % span + 1) * SUB, :] = result
        for h in range(halves):
            send_all(chunks + g * halves + h)
        if assisted:
            @pl.when(is_gate)
            def _():
                at_steps(g, {g: SPREAD[g] for g in SPREAD if g < groups}, spread)

        return carry

    lax.fori_loop(0, groups, opening, 0)
    @pl.when(jnp.logical_not(is_gate))
    def _():
        relay(jnp.int32(chunks + 1), first_relay)

    for s in range(LEAD2):
        relay(jnp.int32(chunks + s), second_relay)

    def place(ch):
        for j in range(1, n_row):
            row_from(ch, j).wait_recv()
        arrived = income[ch].reshape(n_row * m, part)
        placed = jnp.dot(put[ch], arrived, preferred_element_type=F32)
        out_ref[...] = (out_ref[...].astype(F32) + placed).astype(BF16)

    def finish(s, l, ch, result):
        drain_own(s)

        @pl.when(l < layers - 1)
        def _():
            hidden[s + chunks, me_c] = result
            send_all(s + chunks)

        @pl.when(l == layers - 1)
        def _():
            income[ch, me_r] = result
            for j in range(1, n_row):
                row_copy(ch, j).start()

    def after(s, l, ch):
        @pl.when((l == layers - 1) & (ch >= 2))
        def _():
            place(ch - 2)

        @pl.when(s == chunks)
        def _():
            pass_ids()

        @pl.when(s == 2 * chunks)
        def _():
            find_places()

    def step(s, carry):
        l = s // chunks
        ch = s % chunks
        relay(s + LEAD2, second_relay)
        relay(s + LEAD1, first_relay)

        @pl.when((ch == 0) & (l < first_helped) if assisted else ch == 0)
        def _():
            weight_copy(l).wait()

        await_rest(s)
        total = jnp.zeros((m, part), F32)
        for c in range(n_col):
            values = hidden[s, c].astype(F32)
            total = total + values * values
        mean = jnp.sum(total, axis=1, keepdims=True) * (1.0 / width)
        inverse = lax.rsqrt(mean + epsilon)
        for c in range(n_col):
            cols = slice(c * part, (c + 1) * part)
            active[:m, cols] = silu(hidden[s, c].astype(F32) * inverse * gain[l, :, cols])
        update = jnp.dot(active[:m, :], weight[l], preferred_element_type=F32)
        result = (hidden[s, me_c].astype(F32) + update).astype(BF16)
        finish(s, l, ch, result)
        if assisted:
            move_weights(s)
        after(s, l, ch)
        return carry

    near_cols = pl.ds(pl.multiple_of(near_base, width // 2), width // 2)
    far_cols = pl.ds(pl.multiple_of(far_base, width // 2), width // 2)

    def activate(s, l, begin, inverse):
        for q in range(n_col // 2):
            c = begin * (n_col // 2) + q
            cols = columns(c)
            active[:m, cols] = silu(hidden[s, c].astype(F32) * inverse * gain[l, :, cols])

    def helped_step(s, carry):
        l = s // chunks
        ch = s % chunks
        square = lax.broadcasted_iota(jnp.int32, (m, m), 0) == lax.broadcasted_iota(jnp.int32, (m, m), 1)
        relay(s + LEAD2, second_relay)
        relay(s + LEAD1, first_relay)

        @pl.when(ch == 0)
        def _():
            await_weights(l)

        await_helped(s)

        @pl.when(is_gate)
        def _():
            total = jnp.zeros((m, part), F32)
            for c in range(n_col):
                values = hidden[s, c].astype(F32)
                total = total + values * values
            mean = jnp.sum(total, axis=1, keepdims=True) * (1.0 / width)
            inverse = lax.rsqrt(mean + epsilon)

            @pl.when(s >= bound + chunks)
            def _():
                scale_copy(s - chunks).wait_send()
                part_copy(s - chunks).wait_send()

            scale_out[ch, 0:1, 0:m] = jnp.sum(jnp.where(square, inverse, 0.0), axis=0, keepdims=True)
            scale_copy(s).start()
            activate(s, l, 1 - side, inverse)
            theirs = helped[l - first_helped].reshape(width // 2, part)
            part_out[ch] = jnp.dot(active[:m, far_cols], theirs, preferred_element_type=F32).astype(BF16)
            part_copy(s).start()
            activate(s, l, side, inverse)
            update = jnp.dot(active[:m, :], weight[l], preferred_element_type=F32)
            finish(s, l, ch, (hidden[s, me_c].astype(F32) + update).astype(BF16))

        @pl.when(jnp.logical_not(is_gate))
        def _():
            scale_copy(s).wait_recv()
            inverse = jnp.sum(jnp.where(square, scale_in[s - bound, 0:1, 0:m], 0.0), axis=1, keepdims=True)
            activate(s, l, side, inverse)
            update = jnp.dot(active[:m, near_cols], weight[l, near_cols, :], preferred_element_type=F32)
            part_copy(s).wait_recv()
            update = update + part_in[s - bound].astype(F32)
            finish(s, l, ch, (hidden[s, me_c].astype(F32) + update).astype(BF16))

        @pl.when(s == steps - 2)
        def _():
            drain_weights()

        after(s, l, ch)
        return carry

    lax.fori_loop(chunks, bound, step, 0)
    if assisted:
        lax.fori_loop(bound, steps, helped_step, 0)
    for ch in range(chunks):
        first_relay(jnp.int32(steps - chunks + ch), False)
        second_relay(jnp.int32(steps - chunks + ch), False)
    for j in range(1, n_row):
        id_row_copy(j).wait_send()
    for j in range(1, n_col):
        id_col_copy(j).wait_send()
    if assisted:
        @pl.when(is_gate)
        def _():
            for ch in range(chunks):
                scale_copy(steps - chunks + ch).wait_send()
                part_copy(steps - chunks + ch).wait_send()

    for ch in range(chunks - 1):
        for j in range(1, n_row):
            row_copy(ch, j).wait_send()
    place(chunks - 2)
    place(chunks - 1)
    for j in range(1, n_row):
        row_copy(chunks - 1, j).wait_send()


def shards(rows, task_ids, task_embed, norm_gain, layer_weight):
    rows_dev, width = rows.shape
    tasks = task_embed.shape[0]
    layers = layer_weight.shape[0]
    part = layer_weight.shape[2]
    n_row = lax.axis_size("row")
    n_col = lax.axis_size("col")
    slots = rows_dev * n_col
    chunks = CHUNKS
    m = slots // chunks
    lead_dim = -(-n_row // 8) * 8
    lanes = 128
    assisted = 1 if n_col // INNER == 4 and n_row == 4 and chunks == 4 and layers >= 4 and m <= 128 else 0
    sizes = (n_row, n_col, layers, chunks, tasks, assisted)
    spots = max(assisted * chunks, 1)
    buffers = [
        pltpu.VMEM((rows_dev, width), BF16),
        pltpu.VMEM((1, rows_dev), jnp.int32),
        pltpu.VMEM((tasks, width), BF16),
        pltpu.VMEM((layers, 1, width), F32),
        pltpu.VMEM((layers, width, part), BF16),
        pltpu.VMEM((layers * chunks, n_col, m, part), BF16),
        pltpu.VMEM((n_col * SUB, width), BF16),
        pltpu.VMEM((chunks, n_row, m, part), BF16),
        pltpu.VMEM((chunks, slots, n_row * m), BF16),
        pltpu.VMEM((max(assisted, 1), n_row, width // 2 // n_row if assisted else 16, part), BF16),
        pltpu.VMEM((chunks, m, part), BF16),
        pltpu.VMEM((spots, m, part), BF16),
        pltpu.VMEM((chunks, 8, lanes), F32),
        pltpu.VMEM((spots, 8, lanes), F32),
        pltpu.VMEM((lead_dim, lanes), jnp.int32),
        pltpu.VMEM((n_row, lead_dim, lanes), jnp.int32),
        pltpu.VMEM((lead_dim, lanes), jnp.int32),
        pltpu.VMEM((n_col, lead_dim, lanes), jnp.int32),
    ]
    held = sum(math.prod(b.shape) * jnp.dtype(b.dtype).itemsize for b in buffers)
    dma = pltpu.SemaphoreType.DMA
    vmem = pl.BlockSpec(memory_space=pltpu.VMEM)
    hbm = pl.BlockSpec(memory_space=pltpu.HBM)
    operands = [rows, task_ids.reshape(1, rows_dev), task_embed, norm_gain, layer_weight]
    return pl.pallas_call(
        functools.partial(kernel, sizes),
        out_shape=jax.ShapeDtypeStruct((slots, part), BF16),
        in_specs=[hbm] * 5,
        out_specs=vmem,
        scratch_shapes=buffers
        + [
            dma((3,)),
            dma((layers,)),
            dma((layers,)),
            dma((n_row,)),
            dma((n_row,)),
            dma((n_col,)),
            dma((n_col,)),
            dma((chunks, n_row)),
            dma((chunks, n_row)),
            dma((chunks, n_col // INNER // 2 + 1)),
            dma((chunks, n_col // INNER)),
            dma((chunks, n_col // INNER, max(1, n_col // INNER // 2 - 1))),
            dma((2 * chunks, n_col)),
            dma((spots, 4)),
            dma((spots, n_row)),
            dma((chunks,)),
            dma((spots,)),
            dma((chunks,)),
            dma((spots,)),
        ],
        compiler_params=pltpu.CompilerParams(
            collective_id=0, has_side_effects=True, vmem_limit_bytes=min(held + SPARE, 60 * 2**20)
        ),
    )(*[pltpu.with_memory_space_constraint(operand, pltpu.HBM) for operand in operands])


def solution(mesh):
    return jax.shard_map(
        shards,
        mesh=mesh,
        in_specs=(P(("row", "col"), None), P(("row", "col")), P(), P(), P(None, None, "col")),
        out_specs=P("row", "col"),
        check_vma=False,
    )
```

```python
import functools
import math

import jax
import jax.numpy as jnp
from jax import lax
from jax.experimental import pallas as pl
from jax.experimental.pallas import tpu as pltpu
from jax.sharding import PartitionSpec as P

epsilon = 1e-06
MESH = pl.DeviceIdType.MESH
INNER = 2
CHUNKS = 4
SUB = 16
SPARE = 10 * 2**20
LEAD1 = 2
LEAD2 = 1
SHIP = {0: (0,), 1: (1, 2), 5: (3,)}
SPREAD = {1: (0,), 4: (1,), 6: (2,), 9: (3,)}
RELAY = {5: (0,), 6: (1,), 8: (2,), 11: (3,)}
F32 = jnp.float32
BF16 = jnp.bfloat16


def kernel(
    sizes,
    rows_hbm,
    ids_hbm,
    embed_hbm,
    gain_hbm,
    weight_ref,
    out_ref,
    rows_ref,
    ids_ref,
    embed_ref,
    gain,
    weight,
    hidden,
    active,
    income,
    put,
    helped,
    part_out,
    part_in,
    scale_out,
    scale_in,
    id_own,
    id_row,
    id_sum,
    id_col,
    sem_input,
    sem_gain,
    sem_weight,
    send_idrow,
    recv_idrow,
    send_idcol,
    recv_idcol,
    send_row,
    recv_row,
    send_own,
    send_relay,
    send_along,
    recv_hidden,
    send_help,
    recv_help,
    send_part,
    recv_part,
    send_scale,
    recv_scale,
):
    n_row, n_col, layers, chunks, tasks, assisted = sizes
    n_outer = n_col // INNER
    rows_dev = rows_ref.shape[0]
    width = rows_ref.shape[1]
    part = width // n_col
    slots = rows_dev * n_col
    m = slots // chunks
    steps = layers * chunks
    first_helped = layers - assisted
    bound = first_helped * chunks
    groups = rows_dev // SUB
    halves = chunks // groups
    span = n_col // halves
    me_r = lax.axis_index("row")
    me_c = lax.axis_index("col")
    outer = me_c // INNER
    inner = me_c % INNER
    partner = outer * INNER + (INNER - 1 - inner)

    def columns(c):
        return pl.ds(pl.multiple_of(c * part, part), part)

    def col_peer(j):
        return (me_c + j) % n_col

    def row_peer(j):
        return (me_r + j) % n_row

    def remote(src, dst, send, recv, r, c):
        return pltpu.make_async_remote_copy(
            src_ref=src, dst_ref=dst, send_sem=send, recv_sem=recv, device_id=(r, c), device_id_type=MESH
        )

    def weight_copy(l):
        return pltpu.make_async_copy(weight_ref.at[l], weight.at[l], sem_weight.at[l])

    barrier = pltpu.get_barrier_semaphore()
    for j in range(1, n_row):
        pl.semaphore_signal(barrier, inc=1, device_id=(row_peer(j), me_c), device_id_type=MESH)
    for j in range(1, n_col):
        pl.semaphore_signal(barrier, inc=1, device_id=(me_r, col_peer(j)), device_id_type=MESH)

    inputs = [
        pltpu.make_async_copy(source, dest, sem_input.at[i])
        for i, (source, dest) in enumerate(((rows_hbm, rows_ref), (embed_hbm, embed_ref), (ids_hbm, ids_ref)))
    ]
    for copy in inputs:
        copy.start()

    def gain_copy(l):
        return pltpu.make_async_copy(gain_hbm.at[pl.ds(l, 1)], gain.at[l], sem_gain.at[l])

    out_ref[...] = jnp.zeros(out_ref.shape, BF16)
    for copy in inputs:
        copy.wait()
    for l in range(layers):
        gain_copy(l).start()
        weight_copy(l).start()

    lead_dim = id_own.shape[0]
    lanes = id_own.shape[1]
    per_tile = lanes // rows_dev
    raw_ids = ids_ref[...]
    spread = lax.broadcasted_iota(jnp.int32, (rows_dev, lanes), 1) - lax.broadcasted_iota(
        jnp.int32, (rows_dev, lanes), 0
    )
    spread = jnp.where(spread == (me_c % per_tile) * rows_dev, 1.0, 0.0).astype(BF16)
    own_ids = jnp.broadcast_to(raw_ids.astype(F32), (lead_dim, rows_dev)).astype(BF16)
    row_ids = jnp.dot(own_ids, spread, preferred_element_type=F32).astype(jnp.int32)
    sub = lax.broadcasted_iota(jnp.int32, (lead_dim, lanes), 0)
    id_own[...] = jnp.where(sub == me_r, row_ids, 0)

    eye = jnp.where(
        lax.broadcasted_iota(jnp.int32, (rows_dev, rows_dev), 0)
        == lax.broadcasted_iota(jnp.int32, (rows_dev, rows_dev), 1),
        1.0,
        0.0,
    ).astype(BF16)
    tall_ids = lax.dot_general(eye, own_ids, (((1,), (1,)), ((), ())), preferred_element_type=F32)[:, 0:1]
    embed_on = [jnp.where(tall_ids == float(t), 1.0, 0.0) for t in range(tasks)]
    for g in range(groups):
        lines = slice(g * SUB, (g + 1) * SUB)
        for c in range(n_col):
            cols = slice(c * part, (c + 1) * part)
            term = jnp.zeros((SUB, part), F32)
            for t in range(tasks):
                term = term + embed_on[t][lines, :] * embed_ref[t : t + 1, cols].astype(F32)
            begin = (rows_ref[lines, cols].astype(F32) + term).astype(BF16)
            hidden[g * halves + c // span, me_c, (c % span) * SUB : (c % span + 1) * SUB, :] = begin

    pl.semaphore_wait(barrier, n_row + n_col - 2)

    def id_row_copy(j):
        return remote(id_own, id_row.at[me_r], send_idrow.at[j], recv_idrow.at[me_r], row_peer(j), me_c)

    def id_row_from(j):
        return remote(id_own, id_row.at[row_peer(j)], send_idrow.at[j], recv_idrow.at[row_peer(j)], row_peer(j), me_c)

    def id_col_copy(j):
        return remote(id_sum, id_col.at[me_c], send_idcol.at[j], recv_idcol.at[me_c], me_r, col_peer(j))

    def id_col_from(j):
        return remote(id_sum, id_col.at[col_peer(j)], send_idcol.at[j], recv_idcol.at[col_peer(j)], me_r, col_peer(j))

    def row_copy(ch, j):
        block = income.at[ch, me_r]
        return remote(block, block, send_row.at[ch, j], recv_row.at[ch, me_r], row_peer(j), me_c)

    def row_from(ch, j):
        block = income.at[ch, row_peer(j)]
        return remote(block, block, send_row.at[ch, j], recv_row.at[ch, row_peer(j)], row_peer(j), me_c)

    half = n_outer // 2
    side = outer // half
    is_gate = outer == half - 1 + side
    far_gate = (half - side) * INNER + inner

    def near(j, i):
        return (side * half + (outer % half + j) % half) * INNER + i

    def far(k, i):
        return ((1 - side) * half + k) * INNER + i

    other = INNER - 1 - inner

    def block_copy(s, source, send, peer):
        block = hidden.at[s, source]
        return remote(block, block, send, recv_hidden.at[s % (2 * chunks), source], me_r, peer)

    def await_block(s, source):
        block_copy(s, source, send_relay.at[0, 0], partner).wait_recv()

    def near_copies(s):
        return [block_copy(s, me_c, send_own.at[s % chunks, j], near(j, inner)) for j in range(1, half)]

    def other_copies(s):
        return [
            block_copy(s, me_c, send_own.at[s % chunks, half], far_gate),
            block_copy(s, me_c, send_own.at[s % chunks, 0], partner),
        ]

    def own_copies(s):
        return other_copies(s) + near_copies(s)

    def send_all(s):
        for copy in own_copies(s):
            copy.start()

    def drain_own(s):
        for copy in own_copies(s):
            copy.wait_send()

    def over(s, source):
        return block_copy(s, source, send_relay.at[s % chunks, source // INNER], partner)

    def along(s, source, j):
        return block_copy(s, source, send_along.at[s % chunks, source // INNER, j - 1], near(j, inner))

    def across(s, source):
        return block_copy(s, source, send_along.at[s % chunks, source // INNER, 0], far_gate)

    def pass_on(s, go, source, copies):
        if go:
            await_block(s, source)
        for copy in copies:
            if go:
                copy.start()
            else:
                copy.wait_send()

    mate = near(1, inner)
    far_corner = far(1 - side, inner) if half == 2 else far_gate
    even_of = lambda s: s % 2 == 0
    odd_of = lambda s: s % 2 == 1

    def full_first(s, go):
        @pl.when(is_gate)
        def _():
            for k in range(half):
                source = far(k, inner)
                pass_on(s, go, source, [along(s, source, j) for j in range(1, half)] + [over(s, source)])

        @pl.when(even_of(s))
        def _():
            for j in range(1, half):
                pass_on(s, go, near(j, inner), [over(s, near(j, inner))])

        @pl.when(odd_of(s))
        def _():
            pass_on(s, go, partner, [along(s, partner, j) for j in range(1, half)])

    def full_second(s, go):
        @pl.when(jnp.logical_not(is_gate))
        def _():
            for k in range(half):
                pass_on(s, go, far(k, inner), [over(s, far(k, inner))])

    def helped_first(s, go):
        @pl.when(jnp.logical_not(is_gate))
        def _():
            pass_on(s, go, partner, [along(s, partner, 1)])
            pass_on(s, go, mate, [over(s, mate)])

        @pl.when(is_gate)
        def _():
            pass_on(s, go, partner, [across(s, partner)])

    def helped_second(s, go):
        @pl.when(is_gate)
        def _():
            pass_on(s, go, far_corner, [over(s, far_corner)])

    def either(s, full, helped_one, go):
        if not assisted:
            full(s, go)
            return

        @pl.when(s < bound)
        def _():
            full(s, go)

        @pl.when(s >= bound)
        def _():
            helped_one(s, go)

    def first_relay(s, go):
        either(s, full_first, helped_first, go)

    def second_relay(s, go):
        either(s, full_second, helped_second, go)

    def await_rest(s):
        @pl.when(even_of(s))
        def _():
            await_block(s, partner)

        @pl.when(odd_of(s))
        def _():
            for j in range(1, half):
                await_block(s, near(j, inner))

        for j in range(1, half):
            await_block(s, near(j, other))
        for k in range(half):
            await_block(s, far(k, other))

    def await_helped(s):
        await_block(s, near(1, other))

        @pl.when(is_gate)
        def _():
            await_block(s, far_gate)
            await_block(s, mate)
            for k in range(half):
                await_block(s, far(k, other))

    far_base = (1 - side) * (width // 2)
    near_base = side * (width // 2)
    share = width // 2 // n_row
    bite = share // chunks
    sibling = me_r + 1 - 2 * (me_r % 2)
    cross = (me_r + 2) % n_row

    def helped_part(i, q):
        return helped.at[i // chunks, q, pl.ds((i % chunks) * bite, bite), :]

    def ship_copy(i):
        lines = pl.ds(pl.multiple_of(far_base + me_r * share + (i % chunks) * bite, bite), bite)
        source = weight.at[first_helped + i // chunks, lines, :]
        return remote(source, helped_part(i, me_r), send_help.at[i, 0], recv_help.at[i, me_r], me_r, mate)

    def help_copy(i, q, way, peer):
        block = helped_part(i, q)
        return remote(block, block, send_help.at[i, way], recv_help.at[i, q], peer, me_c)

    def spread_copies(i):
        return [help_copy(i, me_r, 1, sibling), help_copy(i, me_r, 2, cross)]

    def part_copy(s):
        slot = s - bound
        return remote(
            part_out.at[s % chunks], part_in.at[slot], send_part.at[s % chunks], recv_part.at[slot], me_r, mate
        )

    def scale_copy(s):
        slot = s - bound
        return remote(
            scale_out.at[s % chunks], scale_in.at[slot], send_scale.at[s % chunks], recv_scale.at[slot], me_r, mate
        )

    def at_steps(s, table, action):
        for when, items in table.items():
            @pl.when(s == when)
            def _():
                for i in items:
                    action(i)

    def spread(i):
        help_copy(i, me_r, 1, sibling).wait_recv()
        for copy in spread_copies(i):
            copy.start()

    def pass_cross(i):
        help_copy(i, cross, 3, sibling).wait_recv()
        help_copy(i, cross, 3, sibling).start()

    def move_weights(s):
        @pl.when(is_gate)
        def _():
            at_steps(s, RELAY, pass_cross)
            at_steps(s, SPREAD, spread)

        @pl.when(jnp.logical_not(is_gate))
        def _():
            at_steps(s, SHIP, lambda i: ship_copy(i).start())

    def await_weights(l):
        for i in range(assisted * chunks):
            @pl.when(is_gate & (l == first_helped + i // chunks))
            def _():
                for q in (sibling, (cross + 1 - 2 * (me_r % 2))):
                    help_copy(i, q, 1, sibling).wait_recv()

    def drain_weights():
        for i in range(assisted * chunks):
            @pl.when(is_gate)
            def _():
                for copy in spread_copies(i) + [help_copy(i, cross, 3, sibling)]:
                    copy.wait_send()

            @pl.when(jnp.logical_not(is_gate))
            def _():
                ship_copy(i).wait_send()

    def relay(s, relay_of):
        @pl.when(s < steps)
        def _():
            @pl.when(s >= chunks)
            def _():
                relay_of(s - chunks, False)

            relay_of(s, True)

    for j in range(1, n_row):
        id_row_copy(j).start()
    def open_sends(ch):
        if ch < chunks - 1:
            send_all(ch)
        else:
            for copy in other_copies(ch):
                copy.start()

            @pl.when(jnp.logical_not(is_gate))
            def _():
                for copy in near_copies(ch):
                    copy.start()

    for ch in range(chunks):
        open_sends(ch)

    for s in range(LEAD1):
        first_relay(jnp.int32(s), True)
    for s in range(LEAD2):
        second_relay(jnp.int32(s), True)

    def pass_ids():
        ids_here = id_own[...]
        for j in range(1, n_row):
            id_row_from(j).wait_recv()
            ids_here = ids_here + id_row[row_peer(j)]
        id_sum[...] = ids_here
        id_col[me_c] = ids_here
        for j in range(1, n_col):
            id_col_copy(j).start()

    def find_places():
        for j in range(1, n_col):
            id_col_from(j).wait_recv()
        tiles = []
        for tile in range(n_col // per_tile):
            joined = id_col[tile * per_tile]
            for c in range(tile * per_tile + 1, (tile + 1) * per_tile):
                joined = joined + id_col[c]
            tiles.append(joined)
        ids = jnp.concatenate(tiles, 1)

        bits = SUB.bit_length() - 1
        wide = (n_col * SUB).bit_length() - 1

        def origin(lane):
            group = lane >> wide
            source = (lane >> bits) & (n_col - 1)
            return source * rows_dev + group * SUB + (lane & (SUB - 1))

        low = lax.broadcasted_iota(jnp.int32, (slots, slots), 0)
        high = lax.broadcasted_iota(jnp.int32, (slots, slots), 1)
        shuffle = jnp.where(low == origin(high), 1.0, 0.0).astype(BF16)
        earlier = jnp.where(origin(low) < origin(high), 1.0, 0.0).astype(BF16)
        ids = jnp.dot(ids.astype(F32).astype(BF16), shuffle, preferred_element_type=F32).astype(jnp.int32)
        line = lax.broadcasted_iota(jnp.int32, (lead_dim, slots), 0)
        line_col = lax.broadcasted_iota(jnp.int32, (lead_dim, 1), 0)
        ids = jnp.where(line < n_row, ids, tasks)
        live = ids < tasks
        member = [jnp.where(ids == t, 1.0, 0.0) for t in range(tasks)]
        ranks = jnp.dot(jnp.concatenate(member, 0).astype(BF16), earlier, preferred_element_type=F32)
        base = jnp.zeros((1, 1), F32)
        position = jnp.zeros((lead_dim, slots), F32)
        for t in range(tasks):
            count = jnp.sum(member[t], axis=1, keepdims=True)
            offset = jnp.zeros((lead_dim, 1), F32) + base
            for r in range(n_row):
                here = count[r : r + 1, :]
                offset = offset + jnp.where(line_col > r, here, 0.0)
                base = base + here
            rank = ranks[t * lead_dim : (t + 1) * lead_dim, :]
            position = position + member[t] * (offset + rank)
        slot = jnp.floor((position + 0.5) * (1.0 / n_row))
        target = jnp.where(live, position - slot * n_row, -1.0).astype(jnp.int32)
        slot = jnp.where(target == me_r, slot.astype(jnp.int32), -1)
        slot_range = lax.broadcasted_iota(jnp.int32, (slots, n_row * m), 0)
        for ch in range(chunks):
            aimed = jnp.concatenate([slot[r : r + 1, ch * m : (ch + 1) * m] for r in range(n_row)], 1)
            put[ch] = jnp.where(slot_range == aimed, 1.0, 0.0).astype(BF16)

    def silu(values):
        half = 0.5 * values
        return (half + half * jnp.tanh(half)).astype(BF16)

    def opening(g, carry):
        if assisted:
            @pl.when(g == 0)
            def _():
                for l in range(first_helped, layers):
                    weight_copy(l).wait()

            @pl.when(jnp.logical_not(is_gate))
            def _():
                at_steps(g, {g: SHIP[g] for g in SHIP if g < groups}, lambda i: ship_copy(i).start())

        @pl.when(g == 0)
        def _():
            for s in range(LEAD1, chunks):
                first_relay(jnp.int32(s), True)

            @pl.when(is_gate)
            def _():
                for copy in near_copies(chunks - 1):
                    copy.start()

            weight_copy(0).wait()
            for l in range(layers):
                gain_copy(l).wait()

        for h in range(halves):
            if h > 0:
                second_relay(g * halves + h, True)
            else:
                @pl.when(g > 0)
                def _():
                    second_relay(g * halves, True)
        for h in range(halves):
            await_rest(g * halves + h)

        @pl.when(g == groups - 1)
        def _():
            relay(jnp.int32(chunks), first_relay)

            @pl.when(is_gate)
            def _():
                relay(jnp.int32(chunks + 1), first_relay)

        for c in range(n_col):
            lines = slice(c * SUB, (c + 1) * SUB)

            def piece(p):
                return hidden[g * halves + p // span, c, (p % span) * SUB : (p % span + 1) * SUB, :].astype(F32)

            total = jnp.zeros((SUB, part), F32)
            for p in range(n_col):
                values = piece(p)
                total = total + values * values
            inverse = lax.rsqrt(jnp.sum(total, axis=1, keepdims=True) * (1.0 / width) + epsilon)
            for p in range(n_col):
                cols = slice(p * part, (p + 1) * part)
                active[lines, cols] = silu(piece(p) * inverse * gain[0, :, cols])
        update = jnp.dot(active[...], weight[0], preferred_element_type=F32)
        own_lines = pl.ds(pl.multiple_of((me_c % span) * SUB, SUB), SUB)
        for h in range(halves):
            drain_own(g * halves + h)
        for c in range(n_col):
            own = hidden[g * halves + me_c // span, c, own_lines, :].astype(F32)
            result = (own + update[c * SUB : (c + 1) * SUB, :]).astype(BF16)
            hidden[chunks + g * halves + c // span, me_c, (c % span) * SUB : (c % span + 1) * SUB, :] = result
        for h in range(halves):
            send_all(chunks + g * halves + h)
        if assisted:
            @pl.when(is_gate)
            def _():
                at_steps(g, {g: SPREAD[g] for g in SPREAD if g < groups}, spread)

        return carry

    lax.fori_loop(0, groups, opening, 0)
    @pl.when(jnp.logical_not(is_gate))
    def _():
        relay(jnp.int32(chunks + 1), first_relay)

    for s in range(LEAD2):
        relay(jnp.int32(chunks + s), second_relay)

    def place(ch):
        for j in range(1, n_row):
            row_from(ch, j).wait_recv()
        arrived = income[ch].reshape(n_row * m, part)
        placed = jnp.dot(put[ch], arrived, preferred_element_type=F32)
        out_ref[...] = (out_ref[...].astype(F32) + placed).astype(BF16)

    def finish(s, l, ch, result):
        drain_own(s)

        @pl.when(l < layers - 1)
        def _():
            hidden[s + chunks, me_c] = result
            send_all(s + chunks)

        @pl.when(l == layers - 1)
        def _():
            income[ch, me_r] = result
            for j in range(1, n_row):
                row_copy(ch, j).start()

    def after(s, l, ch):
        @pl.when(s == chunks)
        def _():
            pass_ids()

        @pl.when(s == 2 * chunks)
        def _():
            find_places()

    def step(s, carry):
        l = s // chunks
        ch = s % chunks
        relay(s + LEAD2, second_relay)
        relay(s + LEAD1, first_relay)

        @pl.when((ch == 0) & (l < first_helped) if assisted else ch == 0)
        def _():
            weight_copy(l).wait()

        await_rest(s)
        total = jnp.zeros((m, part), F32)
        for c in range(n_col):
            values = hidden[s, c].astype(F32)
            total = total + values * values
        mean = jnp.sum(total, axis=1, keepdims=True) * (1.0 / width)
        inverse = lax.rsqrt(mean + epsilon)
        for c in range(n_col):
            cols = slice(c * part, (c + 1) * part)
            active[:m, cols] = silu(hidden[s, c].astype(F32) * inverse * gain[l, :, cols])
        update = jnp.dot(active[:m, :], weight[l], preferred_element_type=F32)
        result = (hidden[s, me_c].astype(F32) + update).astype(BF16)
        finish(s, l, ch, result)
        if assisted:
            move_weights(s)
        after(s, l, ch)
        return carry

    near_cols = pl.ds(pl.multiple_of(near_base, width // 2), width // 2)
    far_cols = pl.ds(pl.multiple_of(far_base, width // 2), width // 2)

    def slot_lines(ch):
        return pl.ds(pl.multiple_of((ch % 2) * m, m), m)

    def own_result(s):
        l = s // chunks
        ch = s % chunks
        update = jnp.dot(active[slot_lines(ch), :], weight[l], preferred_element_type=F32)
        finish(s, l, ch, (hidden[s, me_c].astype(F32) + update).astype(BF16))

    def activate(s, l, begin, inverse):
        lines = slot_lines(s % chunks)
        for q in range(n_col // 2):
            c = begin * (n_col // 2) + q
            cols = columns(c)
            active[lines, cols] = silu(hidden[s, c].astype(F32) * inverse * gain[l, :, cols])

    def helped_step(s, carry):
        l = s // chunks
        ch = s % chunks
        square = lax.broadcasted_iota(jnp.int32, (m, m), 0) == lax.broadcasted_iota(jnp.int32, (m, m), 1)
        relay(s + LEAD2, second_relay)
        relay(s + LEAD1, first_relay)

        @pl.when(ch == 0)
        def _():
            await_weights(l)

        await_helped(s)

        @pl.when(is_gate)
        def _():
            total = jnp.zeros((m, part), F32)
            for c in range(n_col):
                values = hidden[s, c].astype(F32)
                total = total + values * values
            mean = jnp.sum(total, axis=1, keepdims=True) * (1.0 / width)
            inverse = lax.rsqrt(mean + epsilon)

            @pl.when(s >= bound + chunks)
            def _():
                scale_copy(s - chunks).wait_send()
                part_copy(s - chunks).wait_send()

            scale_out[ch, 0:1, 0:m] = jnp.sum(jnp.where(square, inverse, 0.0), axis=0, keepdims=True)
            scale_copy(s).start()
            activate(s, l, 1 - side, inverse)
            theirs = helped[l - first_helped].reshape(width // 2, part)
            part_out[ch] = jnp.dot(active[slot_lines(ch), far_cols], theirs, preferred_element_type=F32).astype(BF16)
            part_copy(s).start()
            activate(s, l, side, inverse)

            @pl.when(s > bound)
            def _():
                own_result(s - 1)

        @pl.when(jnp.logical_not(is_gate))
        def _():
            scale_copy(s).wait_recv()
            inverse = jnp.sum(jnp.where(square, scale_in[s - bound, 0:1, 0:m], 0.0), axis=1, keepdims=True)
            activate(s, l, side, inverse)
            update = jnp.dot(active[slot_lines(ch), near_cols], weight[l, near_cols, :], preferred_element_type=F32)
            part_copy(s).wait_recv()
            update = update + part_in[s - bound].astype(F32)
            finish(s, l, ch, (hidden[s, me_c].astype(F32) + update).astype(BF16))

        @pl.when(s == steps - 2)
        def _():
            drain_weights()

        after(s, l, ch)
        return carry

    lax.fori_loop(chunks, bound, step, 0)
    if assisted:
        lax.fori_loop(bound, steps, helped_step, 0)

        @pl.when(is_gate)
        def _():
            own_result(jnp.int32(steps - 1))

    for ch in range(chunks):
        first_relay(jnp.int32(steps - chunks + ch), False)
        second_relay(jnp.int32(steps - chunks + ch), False)
    for j in range(1, n_row):
        id_row_copy(j).wait_send()
    for j in range(1, n_col):
        id_col_copy(j).wait_send()
    if assisted:
        @pl.when(is_gate)
        def _():
            for ch in range(chunks):
                scale_copy(steps - chunks + ch).wait_send()
                part_copy(steps - chunks + ch).wait_send()

    for ch in range(chunks - 1):
        for j in range(1, n_row):
            row_copy(ch, j).wait_send()
    for ch in range(chunks):
        place(ch)
    for j in range(1, n_row):
        row_copy(chunks - 1, j).wait_send()


def shards(rows, task_ids, task_embed, norm_gain, layer_weight):
    rows_dev, width = rows.shape
    tasks = task_embed.shape[0]
    layers = layer_weight.shape[0]
    part = layer_weight.shape[2]
    n_row = lax.axis_size("row")
    n_col = lax.axis_size("col")
    slots = rows_dev * n_col
    chunks = CHUNKS
    m = slots // chunks
    lead_dim = -(-n_row // 8) * 8
    lanes = 128
    assisted = 1 if n_col // INNER == 4 and n_row == 4 and chunks == 4 and layers >= 4 and m <= 128 else 0
    sizes = (n_row, n_col, layers, chunks, tasks, assisted)
    spots = max(assisted * chunks, 1)
    buffers = [
        pltpu.VMEM((rows_dev, width), BF16),
        pltpu.VMEM((1, rows_dev), jnp.int32),
        pltpu.VMEM((tasks, width), BF16),
        pltpu.VMEM((layers, 1, width), F32),
        pltpu.VMEM((layers, width, part), BF16),
        pltpu.VMEM((layers * chunks, n_col, m, part), BF16),
        pltpu.VMEM((n_col * SUB, width), BF16),
        pltpu.VMEM((chunks, n_row, m, part), BF16),
        pltpu.VMEM((chunks, slots, n_row * m), BF16),
        pltpu.VMEM((max(assisted, 1), n_row, width // 2 // n_row if assisted else 16, part), BF16),
        pltpu.VMEM((chunks, m, part), BF16),
        pltpu.VMEM((spots, m, part), BF16),
        pltpu.VMEM((chunks, 8, lanes), F32),
        pltpu.VMEM((spots, 8, lanes), F32),
        pltpu.VMEM((lead_dim, lanes), jnp.int32),
        pltpu.VMEM((n_row, lead_dim, lanes), jnp.int32),
        pltpu.VMEM((lead_dim, lanes), jnp.int32),
        pltpu.VMEM((n_col, lead_dim, lanes), jnp.int32),
    ]
    held = sum(math.prod(b.shape) * jnp.dtype(b.dtype).itemsize for b in buffers)
    dma = pltpu.SemaphoreType.DMA
    vmem = pl.BlockSpec(memory_space=pltpu.VMEM)
    hbm = pl.BlockSpec(memory_space=pltpu.HBM)
    operands = [rows, task_ids.reshape(1, rows_dev), task_embed, norm_gain, layer_weight]
    return pl.pallas_call(
        functools.partial(kernel, sizes),
        out_shape=jax.ShapeDtypeStruct((slots, part), BF16),
        in_specs=[hbm] * 5,
        out_specs=vmem,
        scratch_shapes=buffers
        + [
            dma((3,)),
            dma((layers,)),
            dma((layers,)),
            dma((n_row,)),
            dma((n_row,)),
            dma((n_col,)),
            dma((n_col,)),
            dma((chunks, n_row)),
            dma((chunks, n_row)),
            dma((chunks, n_col // INNER // 2 + 1)),
            dma((chunks, n_col // INNER)),
            dma((chunks, n_col // INNER, max(1, n_col // INNER // 2 - 1))),
            dma((2 * chunks, n_col)),
            dma((spots, 4)),
            dma((spots, n_row)),
            dma((chunks,)),
            dma((spots,)),
            dma((chunks,)),
            dma((spots,)),
        ],
        compiler_params=pltpu.CompilerParams(
            collective_id=0, has_side_effects=True, vmem_limit_bytes=min(held + SPARE, 60 * 2**20)
        ),
    )(*[pltpu.with_memory_space_constraint(operand, pltpu.HBM) for operand in operands])


def solution(mesh):
    return jax.shard_map(
        shards,
        mesh=mesh,
        in_specs=(P(("row", "col"), None), P(("row", "col")), P(), P(), P(None, None, "col")),
        out_specs=P("row", "col"),
        check_vma=False,
    )
```
